32 devices in a mesh: section: 4 (over z), shard: 8 (over y, x, core).
Axes of the slice: x: 2, y: 2, z: 4, core: 2. Of those that a mesh axis runs over, the one named last changes fastest.
Arguments:
- grad_parts: bfloat16 [4, 8, 256, 8192], P('section', 'shard'), may hold values from -6 to 6
- params: bfloat16 [4, 256, 8192], P('section', 'shard'), may hold values from -6 to 6
- moment_first: float32 [4, 256, 8192], P('section', 'shard'), may hold values from -6 to 6
- moment_second: float32 [4, 256, 8192], P('section', 'shard'), may hold values from 0.5 to 50
- block_layer: int32 [4, 32], P('section', 'shard'), may hold values from 0 to 7, as said below
- block_valid: int32 [4, 32], P('section', 'shard'), may hold values from 0 to 1
- decay: float32 [8], replicated, may hold values from 0.05 to 1
Outputs:
- new_params: bfloat16 [4, 256, 8192], P('section', 'shard')
- new_first: float32 [4, 256, 8192], P('section', 'shard')
- new_second: float32 [4, 256, 8192], P('section', 'shard')
- ratios: float32 [8], replicated
The draws below stay inside these ranges and needn't reach their ends.
Inputs may be any that keep to these rules, and one draw needn't show every extreme that they name: `block_layer`: in every section the live slots come first. One section has all 32 slots live; each other section has between 16 and 32 live slots, and all sections together have 3 * 32. Over the live slots taken section by section in order, layer ids never fall and every layer has exactly 12 live slots; dead slots hold arbitrary layer ids.
All inputs are finite; a program needn't handle non-finite values.
Results may differ from the reference program's by a relative error of at most 0.008.
Values may be sent and summed in bfloat16 or wider, within the bound.
A program may use at most 64 MiB of HBM per device.

```python
import math
import jax
import jax.numpy as jnp
from jax import lax

D = 8192
LAYERS = 8
BLOCK = 8
SECTION_BLK = 32
SECTION_ROWS = 256
LAYER_BLK = 12
N_SECTION = 4
N_SHARD = 8


def layout(key):
    keyed = jax.random.fold_in(key, 11)
    full = SECTION_BLK
    half_blk = SECTION_BLK // 2
    first_count = jax.random.randint(jax.random.fold_in(keyed, 3), (), half_blk, full + 1)
    lower = jnp.maximum(half_blk, full - first_count)
    upper = jnp.minimum(full, 3 * half_blk - first_count)
    second_count = jax.random.randint(jax.random.fold_in(keyed, 4), (), lower, upper + 1)
    third_count = 2 * full - first_count - second_count
    base = jnp.stack([jnp.array(full, jnp.int32), first_count.astype(jnp.int32), second_count.astype(jnp.int32), third_count.astype(jnp.int32)])
    order = jax.random.permutation(jax.random.fold_in(keyed, 1), 4)
    counts = base[order]
    offsets = jnp.cumsum(counts) - counts
    slots = jnp.arange(SECTION_BLK, dtype=jnp.int32)
    valid = slots[None, :] < counts[:, None]
    position = offsets[:, None] + slots[None, :]
    layer = position // LAYER_BLK
    filler = jax.random.randint(jax.random.fold_in(keyed, 2), (4, SECTION_BLK), 0, LAYERS)
    return (jnp.where(valid, layer, filler).astype(jnp.int32), valid.astype(jnp.int32))


def draw_block_layer(key, part):
    return layout(key)[0]


def draw_block_valid(key, part):
    return layout(key)[1]


def strengthened(result, key, source, target, blocks, factor):
    owner, partner = [(jnp.arange(result.shape[dim]) // (result.shape[dim] // blocks)).reshape([-1 if axis == dim else 1 for axis in range(result.ndim)]) for dim in (source, target)]
    chosen = jax.random.permutation(key, blocks)[partner]
    strong = (owner == chosen) | (owner == (partner + blocks // 2) % blocks)
    return jnp.where(strong, factor * result, result)


def level_of(own_key, shape, shards, least, top_value):
    factor_of, own = 1.0, jax.random.fold_in(own_key, 6)
    for axis_at, blocks in shards:
        heights = jnp.exp(jax.random.uniform(jax.random.fold_in(own, axis_at), (blocks,), jnp.float32, least / len(shards), top_value / len(shards)))
        factor_of = factor_of * jnp.repeat(heights, shape[axis_at] // blocks).reshape([-1 if axis == axis_at else 1 for axis in range(len(shape))])
    return factor_of


def centred(stream_key, shape, spread, bound, split=(), kind=jnp.bfloat16):
    loudness = level_of(stream_key, shape, split, -0.22, 0.18) if split else 1.0
    result = jax.random.normal(stream_key, shape, jnp.float32) * spread * loudness
    return jnp.minimum(jnp.maximum(result, -bound), bound).astype(kind)


def noise_with(key, dims, width, bound, pieces, heavy, kind=jnp.bfloat16):
    entries = width * jax.random.normal(key, dims, jnp.float32)
    if pieces:
        entries = entries * level_of(key, dims, pieces, -0.22, 0.18)
    return jnp.clip(strengthened(entries, jax.random.fold_in(key, 3), *heavy), -bound, bound).astype(kind)


def setup_inputs(seed: int = 0) -> dict:
    seeds = jax.random.split(jax.random.key(seed), 8)
    return {
        "grad_parts": noise_with(seeds[0], (N_SECTION, N_SHARD, SECTION_ROWS, D), 1.0, 6.0, ((0, 4), (1, 8)), (1, 2, 8, 2.0)),
        "params": centred(seeds[1], (N_SECTION, SECTION_ROWS, D), 1.0, 6.0, ((0, 4), (1, 8))),
        "moment_first": centred(seeds[2], (N_SECTION, SECTION_ROWS, D), 1.0, 6.0, ((0, 4), (1, 8)), jnp.float32),
        "moment_second": jnp.clip(jnp.exp(math.log(50.0) - 4.6051702 * jax.random.uniform(seeds[3], (N_SECTION, SECTION_ROWS, D), jnp.float32) ** level_of(seeds[3], (N_SECTION, SECTION_ROWS, D), ((0, 4), (1, 8)), -0.2, 0.2)), 0.5, 50.0),
        "block_layer": draw_block_layer(jax.random.fold_in(seeds[7], 71), 0),
        "block_valid": draw_block_valid(jax.random.fold_in(seeds[7], 71), 0),
        "decay": jnp.clip(jnp.exp(jax.random.uniform(seeds[6], (LAYERS,), jnp.float32, math.log(0.05), math.log(1.0))), 0.05, 1.0),
    }


bias_first = 1.0 - 0.9 ** 10
bias_second = 1.0 - 0.99 ** 10

def reference(grad_parts, params, moment_first, moment_second, block_layer, block_valid, decay):

    def add_part(index, running):
        return running + lax.dynamic_index_in_dim(grad_parts, index, 1, keepdims=False).astype(jnp.float32)
    initial = jnp.zeros((grad_parts.shape[0], grad_parts.shape[2], grad_parts.shape[3]), jnp.float32)
    gradient = lax.fori_loop(0, grad_parts.shape[1], add_part, initial)
    first = 0.9 * moment_first + 0.1 * gradient
    second = 0.99 * moment_second + 0.01 * gradient * gradient
    layer_rows = jnp.repeat(block_layer, BLOCK, axis=1)
    valid_rows = jnp.repeat(block_valid, BLOCK, axis=1) > 0
    weights = params.astype(jnp.float32)
    update = first / bias_first / (jnp.sqrt(second / bias_second) + 1e-06) + decay[layer_rows][..., None] * weights
    onehot = jnp.where(valid_rows[..., None] & (layer_rows[..., None] == jnp.arange(LAYERS, dtype=jnp.int32)), 1.0, 0.0).astype(jnp.float32)
    weight_sq = lax.optimization_barrier(jnp.sum(weights * weights, axis=-1))
    update_sq = lax.optimization_barrier(jnp.sum(update * update, axis=-1))
    wsum = jnp.einsum('sr,srl->l', weight_sq, onehot, precision=lax.Precision.HIGHEST)
    usum = jnp.einsum('sr,srl->l', update_sq, onehot, precision=lax.Precision.HIGHEST)
    ratios = jnp.sqrt(wsum / (usum + 1.0))
    row_ratio = ratios[layer_rows]
    stepped = weights - 0.1 * row_ratio[..., None] * update
    new_params = jnp.where(valid_rows[..., None], stepped, weights).astype(jnp.bfloat16)
    new_first = jnp.where(valid_rows[..., None], first, moment_first)
    new_second = jnp.where(valid_rows[..., None], second, moment_second)
    return (new_params, new_first, new_second, ratios)
```

```python
import functools
import math

import jax
import jax.numpy as jnp
from jax import lax
from jax.experimental import pallas as pl
from jax.experimental.pallas import tpu as pltpu
from jax.sharding import PartitionSpec as P

MESH = pl.DeviceIdType.MESH
bias_first = 1.0 - 0.9**10
bias_second = 1.0 - 0.99**10
LANES = 128
CUTS = (2, 7, 17, 27, 32)
ONE_SHOT = True
PARTS = 2


def kernel(
    n_sec, n_y, n_x, cuts,
    g_hbm, p_hbm, m1_hbm, m2_hbm, layer_hbm, valid_hbm, decay_hbm,
    p_v, upd, new1_ref, new2_ref, step_ref, ratio_ref,
    mine, d2d, m1_v, m2_v, r1x, r1y, s1x, s1y, r2x, r2y, xa, ya, tiles, ztiles, layer_ref, valid_ref, decay_ref,
    pair_recv, one_recv, two_recv, raw_recv, t_recv, z_recv, told,
):
    count = len(cuts)
    most = max(n_x, n_y) - 1
    one_shot = ztiles is None
    dma = pltpu.SemaphoreType.DMA
    pl.run_scoped(
        functools.partial(
            body, n_sec, n_y, n_x, cuts, one_shot,
            g_hbm, p_hbm, m1_hbm, m2_hbm, layer_hbm, valid_hbm, decay_hbm,
            p_v, upd, new1_ref, new2_ref, step_ref, ratio_ref,
            mine, d2d, m1_v, m2_v, (r1x, r1y), (s1x, s1y), (r2x, r2y), (xa, ya), tiles, ztiles,
            layer_ref, valid_ref, decay_ref,
            pair_recv, one_recv, two_recv, raw_recv, t_recv, z_recv, told,
        ),
        load_sem=dma((count, 2)),
        state_sem=dma((6,)),
        pair_send=dma((count, 2)),
        one_send=dma((count, 2, most)),
        two_send=dma((count, 2, most)),
        raw_send=dma((2, most)),
        t_send=dma((1,)),
        z_send=dma((1,)),
    )


def body(
    n_sec, n_y, n_x, cuts, one_shot,
    g_hbm, p_hbm, m1_hbm, m2_hbm, layer_hbm, valid_hbm, decay_hbm,
    p_v, upd, new1_ref, new2_ref, step_ref, ratio_ref,
    mine, d2d, m1_v, m2_v, r1, s1, r2, other, tiles, ztiles, layer_ref, valid_ref, decay_ref,
    pair_recv, one_recv, two_recv, raw_recv, t_recv, z_recv, told,
    load_sem, state_sem, pair_send, one_send, two_send, raw_send, t_send, z_send,
):
    rows, cols = p_v.shape
    half = cols // 2
    count = len(cuts)
    n_shard = 2 * n_y * n_x
    sec, me = lax.axis_index("section"), lax.axis_index("shard")
    core = lax.rem(me, 2)
    x = lax.rem(me // 2, n_x)
    y = me // (2 * n_x)
    blocks = layer_ref.shape[1]
    block_rows = rows // blocks

    def at(yy, xx, cc):
        return (sec, (yy * n_x + xx) * 2 + cc)

    starts = (0,) + cuts[:-1]

    def span(k, d):
        return pl.ds(d * half + starts[k], cuts[k] - starts[k])

    def inner(k):
        return pl.ds(starts[k], cuts[k] - starts[k])

    loads = {}
    for k in range(count):
        for d in range(2):
            c = pltpu.make_async_copy(
                g_hbm.at[:, :, :, :, span(k, d)], mine.at[:, :, :, :, span(k, d)], load_sem.at[k, d]
            )
            c.start()
            loads[k, d] = c
        if k == 0:
            barrier = pltpu.get_barrier_semaphore()
            near = [at(y, x, 1 - core)]
            for cc in (core, 1 - core):
                near += [at(y, lax.rem(x + j, n_x), cc) for j in range(1, n_x)]
                near += [at(lax.rem(y + j, n_y), x, cc) for j in range(1, n_y)]
            for peer in near:
                pl.semaphore_signal(barrier, inc=1, device_id=peer, device_id_type=MESH)
            last_sec = n_sec - 1
            up = (jnp.minimum(sec + 1, last_sec), me)
            down = (jnp.maximum(sec - 1, 0), me)

            @pl.when(sec < last_sec)
            def _():
                pl.semaphore_signal(barrier, inc=1, device_id=up, device_id_type=MESH)

            @pl.when(sec > 0)
            def _():
                pl.semaphore_signal(barrier, inc=1, device_id=down, device_id_type=MESH)

    states = [
        pltpu.make_async_copy(src, dst, state_sem.at[i])
        for i, (src, dst) in enumerate(
            (
                (layer_hbm, layer_ref), (valid_hbm, valid_ref), (decay_hbm, decay_ref),
                (p_hbm, p_v), (m1_hbm, m1_v), (m2_hbm, m2_v),
            )
        )
    ]
    for s in states:
        s.start()

    ends = jnp.where(sec < last_sec, 1, 0) + jnp.where(sec > 0, 1, 0)
    with jax.named_scope("bar"):
        pl.semaphore_wait(barrier, len(near) + ends)

    def relay(d):
        if 1 < d <= n_sec:

            @pl.when(sec >= d - 1)
            def _():
                pl.semaphore_wait(told.at[0, d - 2], 1)

            @pl.when(sec <= n_sec - d)
            def _():
                pl.semaphore_wait(told.at[1, d - 2], 1)

        if d < n_sec:

            @pl.when((sec >= d - 1) & (sec < last_sec))
            def _():
                pl.semaphore_signal(told.at[0, d - 1], inc=1, device_id=up, device_id_type=MESH)

            @pl.when((sec <= n_sec - d) & (sec > 0))
            def _():
                pl.semaphore_signal(told.at[1, d - 1], inc=1, device_id=down, device_id_type=MESH)

    def place(d, t):
        return (slice(None), t) if d == 0 else (t, slice(None))

    def peer_at(d, t, cc):
        return at(y, t, cc) if d == 0 else at(t, x, cc)

    here = (x, y)
    first_n, second_n = (n_x, n_y), (n_y, n_x)

    ones = {(k, d): [] for k in range(count) for d in range(2)}
    raws = {0: [], 1: []}
    for d in range(2):
        with jax.named_scope(f"ldw0{d}"):
            loads[0, d].wait()
        for j in range(1, first_n[d]):
            t = lax.rem(here[d] + j, first_n[d])
            c = pltpu.make_async_remote_copy(
                src_ref=mine.at[(*place(d, t), core, slice(None), span(0, d))],
                dst_ref=r1[d].at[j - 1, :, :, inner(0)],
                send_sem=one_send.at[0, d, j - 1], recv_sem=one_recv.at[0, d, j - 1],
                device_id=peer_at(d, t, core), device_id_type=MESH,
            )
            c.start()
            ones[0, d].append(c)
            c = pltpu.make_async_remote_copy(
                src_ref=mine.at[(*place(d, t), 1 - core, slice(None), span(0, d))],
                dst_ref=other[d].at[j - 1],
                send_sem=raw_send.at[d, j - 1], recv_sem=raw_recv.at[d, j - 1],
                device_id=peer_at(d, t, 1 - core), device_id_type=MESH,
            )
            c.start()
            raws[d].append(c)

    pair = {}

    def send_pair(k, d):
        if k:
            with jax.named_scope(f"ldw{k}{d}"):
                loads[k, d].wait()
        t = slice(None) if k else here[d]
        spot = place(d, t)
        c = pltpu.make_async_remote_copy(
            src_ref=mine.at[(*spot, 1 - core, slice(None), span(k, d))],
            dst_ref=d2d.at[(*spot, slice(None), span(k, d))],
            send_sem=pair_send.at[k, d], recv_sem=pair_recv.at[k, d],
            device_id=at(y, x, 1 - core), device_id_type=MESH,
        )
        c.start()
        pair[k, d] = c

    def add_pair(yy, xx, cut):
        total = mine[yy, xx, core, :, cut].astype(jnp.float32) + d2d[yy, xx, :, cut].astype(jnp.float32)
        mine[yy, xx, core, :, cut] = total.astype(jnp.bfloat16)

    def send_one(k, d):
        with jax.named_scope(f"pairw{k}{d}"):
            pair[k, d].wait_recv()
        cut = span(k, d)

        def add_all(i, carry):
            add_pair(i // n_x, lax.rem(i, n_x), cut)
            return carry

        lax.fori_loop(0, n_y * n_x, add_all, 0)
        for j in range(1, first_n[d]):
            t = lax.rem(here[d] + j, first_n[d])
            c = pltpu.make_async_remote_copy(
                src_ref=mine.at[(*place(d, t), core, slice(None), cut)],
                dst_ref=r1[d].at[j - 1, :, :, inner(k)],
                send_sem=one_send.at[k, d, j - 1], recv_sem=one_recv.at[k, d, j - 1],
                device_id=peer_at(d, t, core), device_id_type=MESH,
            )
            c.start()
            ones[k, d].append(c)

    ahead = 2
    for k in range(1, 1 + ahead):
        for d in range(2):
            send_pair(k, d)
    for d in range(2):
        send_pair(0, d)
    for k in range(1, count):
        for d in range(2):
            send_one(k, d)
        if k + ahead < count:
            for d in range(2):
                send_pair(k + ahead, d)
    for d in range(2):
        pair[0, d].wait_recv()
        for i in range(second_n[d]):
            add_pair(i if d == 0 else y, x if d == 0 else i, span(0, d))

    def partial(k, d, t, cut, near_cut, raw_cut):
        yy, xx = (t, x) if d == 0 else (y, t)
        total = mine[yy, xx, core, :, cut].astype(jnp.float32)
        for i in range(first_n[d] - 1):
            total += r1[d][i, t, :, near_cut].astype(jnp.float32)
            if k == 0:
                total += other[d][i, t, :, raw_cut].astype(jnp.float32)
        return total

    twos = {}
    for k in range(count):
        for d in range(2):
            with jax.named_scope(f"onew{k}{d}"):
                for c in ones[k, d]:
                    c.wait_recv()
                if k == 0:
                    for c in raws[d]:
                        c.wait_recv()
            group = []
            for j in range(1, second_n[d]):
                at_hand = y if d == 0 else x
                t = lax.rem(at_hand + j, second_n[d])
                total = partial(k, d, t, span(k, d), inner(k), slice(None))
                s1[d][j - 1, :, inner(k)] = total.astype(jnp.bfloat16)
                c = pltpu.make_async_remote_copy(
                    src_ref=s1[d].at[j - 1, :, inner(k)], dst_ref=r2[d].at[j - 1, :, inner(k)],
                    send_sem=two_send.at[k, d, j - 1], recv_sem=two_recv.at[k, d, j - 1],
                    device_id=peer_at(1 - d, t, core), device_id_type=MESH,
                )
                c.start()
                group.append(c)
            twos[k, d] = group
        if k < n_sec:
            relay(k + 1)
    for k in range(count, n_sec):
        relay(k + 1)

    def by_block(scalars):
        return jnp.concatenate([jnp.full((block_rows, LANES), s) for s in scalars], axis=0)

    for s in states:
        s.wait()
    layers = [layer_ref[0, b] for b in range(blocks)]
    lives = [valid_ref[0, b] for b in range(blocks)]
    row_decay = by_block([decay_ref[layer] for layer in layers])
    row_live = by_block([jnp.where(v > 0, 1.0, 0.0).astype(jnp.float32) for v in lives]) > 0.5
    for d in range(2):
        for c in raws[d]:
            c.wait_send()
    for k in range(count):
        for d in range(2):
            pair[k, d].wait_send()

    zero = jnp.zeros((rows, LANES), jnp.float32)
    sums = (zero, zero)
    for k in range(count):
        for d in range(2):
            with jax.named_scope(f"twow{k}{d}"):
                for c in twos[k, d]:
                    c.wait_recv()

            def update_piece(i, sums, k=k, d=d):
                usum, wsum = sums
                raw_cut = pl.ds(pl.multiple_of(i * LANES, LANES), LANES)
                near_cut = pl.ds(pl.multiple_of(starts[k] + i * LANES, LANES), LANES)
                cut = pl.ds(pl.multiple_of(d * half + starts[k] + i * LANES, LANES), LANES)
                grad = partial(k, d, y if d == 0 else x, cut, near_cut, raw_cut)
                for j in range(second_n[d] - 1):
                    grad += r2[d][j, :, near_cut].astype(jnp.float32)
                weights = p_v[:, cut].astype(jnp.float32)
                old1, old2 = m1_v[:, cut], m2_v[:, cut]
                first = 0.9 * old1 + 0.1 * grad
                second = 0.99 * old2 + 0.01 * grad * grad
                update = first * (1.0 / bias_first) / (jnp.sqrt(second * (1.0 / bias_second)) + 1e-06)
                update += row_decay * weights
                upd[:, cut] = update
                new1_ref[:, cut] = jnp.where(row_live, first, old1)
                new2_ref[:, cut] = jnp.where(row_live, second, old2)
                return usum + update * update, wsum + weights * weights

            n = (cuts[k] - starts[k]) // LANES
            with jax.named_scope(f"upd{k}{d}"):
                sums = lax.fori_loop(0, n, update_piece, sums, unroll=2 if n % 2 == 0 else 1)

    n_layer = decay_ref.shape[0]
    lane = lax.broadcasted_iota(jnp.int32, (1, LANES), 1)
    lines = []
    for b in range(blocks):
        chosen = jnp.where(lives[b] > 0, layers[b], -LANES)
        for q, values in enumerate((sums[1], sums[0])):
            block = values[b * block_rows : (b + 1) * block_rows]
            lines.append(jnp.where(lane == chosen + q * n_layer, jnp.sum(block, axis=1, keepdims=True), 0.0))
    line = jnp.sum(sum(lines[1:], lines[0]), axis=0, keepdims=True)

    def all_sum(line, slots, send_sem, recv_sem, index, peers):
        slots[index] = line
        for peer in peers:
            pltpu.make_async_remote_copy(
                src_ref=slots.at[index], dst_ref=slots.at[index],
                send_sem=send_sem.at[0], recv_sem=recv_sem.at[0],
                device_id=peer, device_id_type=MESH,
            ).start()
        whole = slots.at[pl.ds(0, len(peers))]
        both = pltpu.make_async_remote_copy(
            src_ref=whole, dst_ref=whole, send_sem=send_sem.at[0], recv_sem=recv_sem.at[0],
            device_id=peers[0], device_id_type=MESH,
        )
        with jax.named_scope("allw"):
            both.wait_recv()
        terms = [slots[j] for j in range(len(peers) + 1)]
        while len(terms) > 1:
            terms = [sum(terms[i + 1 : i + 2], terms[i]) for i in range(0, len(terms), 2)]
        return terms[0], both

    if one_shot:
        every = [
            (lax.rem(sec + i, n_sec), lax.rem(me + j, n_shard))
            for i in (*range(1, n_sec), 0) for j in range(n_shard) if i or j
        ]
        line, sent = all_sum(line, tiles, t_send, t_recv, sec * n_shard + me, every)
        sends = [sent]
    else:
        shard_peers = [(sec, lax.rem(me + j, n_shard)) for j in range(1, n_shard)]
        sec_peers = [(lax.rem(sec + j, n_sec), me) for j in range(1, n_sec)]
        line, sent = all_sum(line, tiles, t_send, t_recv, me, shard_peers)
        line, zsent = all_sum(line, ztiles, z_send, z_recv, sec, sec_peers)
        sends = [sent, zsent]
    ratios = jnp.sqrt(line / (pltpu.roll(line, LANES - n_layer, 1) + 1.0))
    ratio_ref[...] = ratios[0, :n_layer]
    step_ref[...] = jnp.concatenate(
        [
            jnp.broadcast_to(
                0.1 * jnp.sum(
                    jnp.where((lane == layers[b]) & (lives[b] > 0), ratios, 0.0), axis=1, keepdims=True
                ),
                (block_rows, LANES),
            )
            for b in range(blocks)
        ],
        axis=0,
    )
    with jax.named_scope("endw"):
        for group in (*ones.values(), *twos.values(), sends):
            for c in group:
                c.wait_send()


def finish(parts, p_v, upd, new1_v, new2_v, step_v, ratio_v, newp_hbm, new1_hbm, new2_hbm, ratio_hbm, newp_v, sem):
    cols = p_v.shape[1]
    width = cols // parts
    copies = []
    for i, (src, dst) in enumerate(((ratio_v, ratio_hbm), (new1_v, new1_hbm), (new2_v, new2_hbm))):
        c = pltpu.make_async_copy(src, dst, sem.at[i])
        c.start()
        copies.append(c)
    row_step = step_v[...]

    for k in range(parts):
        def step_piece(i, carry, k=k):
            outer = pl.ds(pl.multiple_of(k * width + i * LANES, LANES), LANES)
            stepped = p_v[:, outer].astype(jnp.float32) - row_step * upd[:, outer]
            newp_v[:, outer] = stepped.astype(jnp.bfloat16)
            return carry

        lax.fori_loop(0, width // LANES, step_piece, 0, unroll=4)
        span = pl.ds(k * width, width)
        c = pltpu.make_async_copy(newp_v.at[:, span], newp_hbm.at[:, span], sem.at[3 + k])
        c.start()
        copies.append(c)
    for c in copies:
        c.wait()


def shards(grad_parts, params, moment_first, moment_second, block_layer, block_valid, decay):
    n_sec, n_shard = lax.axis_size("section"), lax.axis_size("shard")
    chips = n_shard // 2
    n_y = max(d for d in range(1, math.isqrt(chips) + 1) if chips % d == 0)
    n_x = chips // n_y
    rows, cols = params.shape[1:]
    n_layer = decay.shape[0]
    half = cols // 2
    cuts = tuple(half // LANES * c // CUTS[-1] * LANES for c in CUTS)
    count = len(cuts)
    bf16, f32 = jnp.bfloat16, jnp.float32
    dma = pltpu.SemaphoreType.DMA
    one_shot = ONE_SHOT and n_shard * n_sec <= 32
    n_lines = n_shard * n_sec if one_shot else n_shard
    most = max(n_x, n_y) - 1
    grads = grad_parts.reshape(n_y, n_x, 2, rows, cols)
    any_spec = pl.BlockSpec(memory_space=pltpu.HBM)
    vmem = pl.BlockSpec(memory_space=pltpu.VMEM)
    held = pl.pallas_call(
        functools.partial(kernel, n_sec, n_y, n_x, cuts),
        out_shape=(
            pltpu.VMEM((rows, cols), bf16),
            pltpu.VMEM((rows, cols), f32),
            pltpu.VMEM((rows, cols), f32),
            pltpu.VMEM((rows, cols), f32),
            pltpu.VMEM((rows, LANES), f32),
            pltpu.VMEM((n_layer,), f32),
        ),
        in_specs=[any_spec] * 7,
        out_specs=(vmem,) * 6,
        scratch_shapes=[
            pltpu.VMEM((n_y, n_x, 2, rows, cols), bf16),
            pltpu.VMEM((n_y, n_x, rows, cols), bf16),
            pltpu.VMEM((rows, cols), f32),
            pltpu.VMEM((rows, cols), f32),
            pltpu.VMEM((n_x - 1, n_y, rows, half), bf16),
            pltpu.VMEM((n_y - 1, n_x, rows, half), bf16),
            pltpu.VMEM((n_y - 1, rows, half), bf16),
            pltpu.VMEM((n_x - 1, rows, half), bf16),
            pltpu.VMEM((n_y - 1, rows, half), bf16),
            pltpu.VMEM((n_x - 1, rows, half), bf16),
            pltpu.VMEM((n_x - 1, n_y, rows, cuts[0]), bf16),
            pltpu.VMEM((n_y - 1, n_x, rows, cuts[0]), bf16),
            pltpu.VMEM((n_lines, 1, LANES), f32),
            None if one_shot else pltpu.VMEM((n_sec, 1, LANES), f32),
            pltpu.SMEM(block_layer.shape, jnp.int32),
            pltpu.SMEM(block_valid.shape, jnp.int32),
            pltpu.SMEM(decay.shape, f32),
            dma((count, 2)),
            dma((count, 2, most)),
            dma((count, 2, most)),
            dma((2, most)),
            dma((1,)),
            dma((1,)),
            pltpu.SemaphoreType.REGULAR((2, n_sec - 1)),
        ],
        compiler_params=pltpu.CompilerParams(
            collective_id=0, has_side_effects=True, vmem_limit_bytes=56 * 1024 * 1024
        ),
    )(grads, params[0], moment_first[0], moment_second[0], block_layer, block_valid, decay)
    out = pl.pallas_call(
        functools.partial(finish, PARTS),
        out_shape=(
            jax.ShapeDtypeStruct((rows, cols), bf16),
            jax.ShapeDtypeStruct((rows, cols), f32),
            jax.ShapeDtypeStruct((rows, cols), f32),
            jax.ShapeDtypeStruct((n_layer,), f32),
        ),
        in_specs=[vmem] * 6,
        out_specs=(any_spec,) * 4,
        scratch_shapes=[pltpu.VMEM((rows, cols), bf16), dma((3 + PARTS,))],
        compiler_params=pltpu.CompilerParams(vmem_limit_bytes=8 * 1024 * 1024),
    )(*held)
    return (out[0][None], out[1][None], out[2][None], out[3])


def solution(mesh):
    placed = (
        P("section", "shard", None, None),
        P("section", "shard", None),
        P("section", "shard", None),
        P("section", "shard", None),
        P("section", "shard"),
        P("section", "shard"),
        P(),
    )
    return jax.shard_map(
        shards,
        mesh=mesh,
        in_specs=placed,
        out_specs=(
            P("section", "shard", None),
            P("section", "shard", None),
            P("section", "shard", None),
            P(),
        ),
        check_vma=False,
    )
```

```python
import functools
import math

import jax
import jax.numpy as jnp
from jax import lax
from jax.experimental import pallas as pl
from jax.experimental.pallas import tpu as pltpu
from jax.sharding import PartitionSpec as P

MESH = pl.DeviceIdType.MESH
bias_first = 1.0 - 0.9**10
bias_second = 1.0 - 0.99**10
root_second = math.sqrt(bias_second)
LANES = 128
CUTS = (2, 4, 7, 15, 23, 29, 31, 32)
SHIFT = 2
ONE_SHOT = True
PARTS = 4


def kernel(
    n_sec, n_y, n_x, cuts,
    g_hbm, p_hbm, m1_hbm, m2_hbm, layer_hbm, valid_hbm, decay_hbm,
    p_v, upd, new1_ref, new2_ref, step_ref, ratio_ref,
    mine, d2d, m1_v, m2_v, r1x, r1y, s1x, s1y, r2x, r2y, xa, ya, xs, ys, tiles, ztiles, layer_ref, valid_ref, decay_ref,
):
    count = len(cuts)
    most = max(n_x, n_y) - 1
    one_shot = ztiles is None
    dma = pltpu.SemaphoreType.DMA
    pl.run_scoped(
        functools.partial(
            body, n_sec, n_y, n_x, cuts, one_shot,
            g_hbm, p_hbm, m1_hbm, m2_hbm, layer_hbm, valid_hbm, decay_hbm,
            p_v, upd, new1_ref, new2_ref, step_ref, ratio_ref,
            mine, d2d, m1_v, m2_v, (r1x, r1y), (s1x, s1y), (r2x, r2y), (xa, ya), (xs, ys), tiles, ztiles,
            layer_ref, valid_ref, decay_ref,
        ),
        load_sem=dma((count, 2)),
        state_sem=dma((6,)),
        pair_send=dma((count, 2)),
        one_send=dma((count, 2, most)),
        two_send=dma((count, 2, most)),
        raw_send=dma((2, 2, most)),
        lent_send=dma((2, 2, most)),
        lent_recv=dma((2, most)),
        t_send=dma((1,)),
        z_send=dma((1,)),
        pair_recv=dma((count, 2)),
        one_recv=dma((count, 2, most)),
        two_recv=dma((count, 2, most)),
        raw_recv=dma((2, most)),
        t_recv=dma((1,)),
        z_recv=dma((1,)),
        told=pltpu.SemaphoreType.REGULAR((2, n_sec - 1)),
    )


def body(
    n_sec, n_y, n_x, cuts, one_shot,
    g_hbm, p_hbm, m1_hbm, m2_hbm, layer_hbm, valid_hbm, decay_hbm,
    p_v, upd, new1_ref, new2_ref, step_ref, ratio_ref,
    mine, d2d, m1_v, m2_v, r1, s1, r2, other, lent, tiles, ztiles, layer_ref, valid_ref, decay_ref,
    load_sem, state_sem, pair_send, one_send, two_send, raw_send, lent_send, lent_recv, t_send, z_send,
    pair_recv, one_recv, two_recv, raw_recv, t_recv, z_recv, told,
):
    rows, cols = p_v.shape
    half = cols // 2
    count = len(cuts)
    n_shard = 2 * n_y * n_x
    sec, me = lax.axis_index("section"), lax.axis_index("shard")
    core = lax.rem(me, 2)
    x = lax.rem(me // 2, n_x)
    y = me // (2 * n_x)
    blocks = layer_ref.shape[1]
    block_rows = rows // blocks

    def at(yy, xx, cc):
        return (sec, (yy * n_x + xx) * 2 + cc)

    starts = (0,) + cuts[:-1]

    def span(k, d):
        return pl.ds(d * half + starts[k], cuts[k] - starts[k])

    def inner(k):
        return pl.ds(starts[k], cuts[k] - starts[k])

    loads = {}
    for k in range(count):
        for d in range(2):
            c = pltpu.make_async_copy(
                g_hbm.at[:, :, :, :, span(k, d)], mine.at[:, :, :, :, span(k, d)], load_sem.at[k, d]
            )
            c.start()
            loads[k, d] = c
        if k == 0:
            barrier = pltpu.get_barrier_semaphore()
            near = [at(y, x, 1 - core)]
            for cc in (core, 1 - core):
                near += [at(y, lax.rem(x + j, n_x), cc) for j in range(1, n_x)]
                near += [at(lax.rem(y + j, n_y), x, cc) for j in range(1, n_y)]
            for peer in near:
                pl.semaphore_signal(barrier, inc=1, device_id=peer, device_id_type=MESH)
            last_sec = n_sec - 1
            up = (jnp.minimum(sec + 1, last_sec), me)
            down = (jnp.maximum(sec - 1, 0), me)

            @pl.when(sec < last_sec)
            def _():
                pl.semaphore_signal(barrier, inc=1, device_id=up, device_id_type=MESH)

            @pl.when(sec > 0)
            def _():
                pl.semaphore_signal(barrier, inc=1, device_id=down, device_id_type=MESH)

    states = [
        pltpu.make_async_copy(src, dst, state_sem.at[i])
        for i, (src, dst) in enumerate(
            (
                (layer_hbm, layer_ref), (valid_hbm, valid_ref), (decay_hbm, decay_ref),
                (p_hbm, p_v), (m1_hbm, m1_v), (m2_hbm, m2_v),
            )
        )
    ]
    for s in states:
        s.start()

    ends = jnp.where(sec < last_sec, 1, 0) + jnp.where(sec > 0, 1, 0)
    with jax.named_scope("bar"):
        pl.semaphore_wait(barrier, len(near) + ends)

    def relay(d):
        if 1 < d <= n_sec:

            @pl.when(sec >= d - 1)
            def _():
                pl.semaphore_wait(told.at[0, d - 2], 1)

            @pl.when(sec <= n_sec - d)
            def _():
                pl.semaphore_wait(told.at[1, d - 2], 1)

        if d < n_sec:

            @pl.when((sec >= d - 1) & (sec < last_sec))
            def _():
                pl.semaphore_signal(told.at[0, d - 1], inc=1, device_id=up, device_id_type=MESH)

            @pl.when((sec <= n_sec - d) & (sec > 0))
            def _():
                pl.semaphore_signal(told.at[1, d - 1], inc=1, device_id=down, device_id_type=MESH)

    def place(d, t):
        return (slice(None), t) if d == 0 else (t, slice(None))

    def peer_at(d, t, cc):
        return at(y, t, cc) if d == 0 else at(t, x, cc)

    here = (x, y)
    first_n, second_n = (n_x, n_y), (n_y, n_x)

    def others(d):
        return [(j, lax.rem(here[d] + j, first_n[d])) for j in range(1, first_n[d])]

    def remote(src, dst, send_sem, recv_sem, peer):
        return pltpu.make_async_remote_copy(
            src_ref=src, dst_ref=dst, send_sem=send_sem, recv_sem=recv_sem, device_id=peer, device_id_type=MESH
        )

    def rows_of(d, t, cc, k):
        return mine.at[(*place(d, t), cc, slice(None), span(k, d))]

    ones, raws, forwards, lends, crosses, pair, kept = {}, {}, {}, {}, {}, {}, {}
    for d in range(2):
        for k in range(count):
            ones[k, d] = [
                remote(
                    rows_of(d, t, core, k), r1[d].at[j - 1, :, :, inner(k)],
                    one_send.at[k, d, j - 1], one_recv.at[k, d, j - 1], peer_at(d, t, core),
                )
                for j, t in others(d)
            ]
            for group, t in ((pair, slice(None)), (kept, here[d])):
                if group is kept and k not in (0, SHIFT):
                    continue
                spot = place(d, t)
                group[k, d] = remote(
                    rows_of(d, t, 1 - core, k), d2d.at[(*spot, slice(None), span(k, d))],
                    pair_send.at[k, d], pair_recv.at[k, d], at(y, x, 1 - core),
                )
        raws[d] = [
            remote(
                rows_of(d, t, 1 - core, 0), other[d].at[j - 1],
                raw_send.at[0, d, j - 1], raw_recv.at[d, j - 1], peer_at(d, t, 1 - core),
            )
            for j, t in others(d)
        ]
        forwards[d] = [
            remote(
                d2d.at[(*place(d, t), slice(None), span(0, d))], other[d].at[j - 1],
                raw_send.at[1, d, j - 1], raw_recv.at[d, j - 1], peer_at(d, t, core),
            )
            for j, t in others(d)
        ]
        lends[d] = [
            remote(
                rows_of(d, t, core, SHIFT), lent[d].at[j - 1],
                lent_send.at[0, d, j - 1], lent_recv.at[d, j - 1], at(y, x, 1 - core),
            )
            for j, t in others(d)
        ]
        crosses[d] = [
            remote(
                rows_of(d, t, 1 - core, SHIFT), r1[d].at[j - 1, :, :, inner(SHIFT)],
                lent_send.at[1, d, j - 1], one_recv.at[SHIFT, d, j - 1], peer_at(d, t, 1 - core),
            )
            for j, t in others(d)
        ]
    is_far, is_near = core == 0, core == 1

    for d in range(2):
        with jax.named_scope(f"ldw0{d}"):
            loads[0, d].wait()
        for c in ones[0, d]:
            c.start()

        @pl.when(is_near)
        def _(d=d):
            for c in raws[d]:
                c.start()

    def send_pair(k, d):
        if k:
            with jax.named_scope(f"ldw{k}{d}"):
                loads[k, d].wait()
        if k in (0, SHIFT):

            @pl.when(is_far)
            def _():
                pair[k, d].start()
                if k:
                    for c in lends[d]:
                        c.start()

            @pl.when(is_near)
            def _():
                kept[k, d].start()
        else:
            pair[k, d].start()

    def add_pair(yy, xx, cut):
        total = mine[yy, xx, core, :, cut].astype(jnp.float32) + d2d[yy, xx, :, cut].astype(jnp.float32)
        mine[yy, xx, core, :, cut] = total.astype(jnp.bfloat16)

    def add_all(cut):
        def add_one(i, carry):
            add_pair(i // n_x, lax.rem(i, n_x), cut)
            return carry

        lax.fori_loop(0, n_y * n_x, add_one, 0)

    def add_kept(d, cut):
        for i in range(second_n[d]):
            add_pair(i if d == 0 else y, x if d == 0 else i, cut)

    def send_one(k, d):
        cut = span(k, d)
        if k == 0:

            @pl.when(is_near)
            def _():
                pair[k, d].wait_recv()
                for c in forwards[d]:
                    c.start()

            @pl.when(is_far)
            def _():
                kept[k, d].wait_recv()

            add_kept(d, cut)
        elif k == SHIFT:

            @pl.when(is_near)
            def _():
                pair[k, d].wait_recv()
                for c in lends[d]:
                    c.wait_recv()
                add_all(cut)
                for c in ones[k, d]:
                    c.start()
                for j, t in others(d):
                    for i in range(second_n[d]):
                        yy, xx = (i, t) if d == 0 else (t, i)
                        total = mine[yy, xx, 1 - core, :, cut].astype(jnp.float32)
                        total += lent[d][j - 1, i].astype(jnp.float32)
                        mine[yy, xx, 1 - core, :, cut] = total.astype(jnp.bfloat16)
                for c in crosses[d]:
                    c.start()

            @pl.when(is_far)
            def _():
                kept[k, d].wait_recv()
                add_kept(d, cut)
        else:
            with jax.named_scope(f"pairw{k}{d}"):
                pair[k, d].wait_recv()
            add_all(cut)
            for c in ones[k, d]:
                c.start()

    ahead = 4
    order = [1, 0, *range(2, count)]
    for k in order[: 1 + ahead]:
        for d in range(2):
            send_pair(k, d)
    for i, k in enumerate(order):
        for d in range(2):
            send_one(k, d)
        if i + 1 + ahead < count:
            for d in range(2):
                send_pair(order[i + 1 + ahead], d)

    def partial(k, d, t, cut, near_cut, raw_cut):
        yy, xx = (t, x) if d == 0 else (y, t)
        total = mine[yy, xx, core, :, cut].astype(jnp.float32)
        for i in range(first_n[d] - 1):
            total += r1[d][i, t, :, near_cut].astype(jnp.float32)
            if k == 0:
                total += other[d][i, t, :, raw_cut].astype(jnp.float32)
        return total

    twos = {}
    for k in range(count):
        for d in range(2):
            with jax.named_scope(f"onew{k}{d}"):
                for c in ones[k, d]:
                    c.wait_recv()
                if k == 0:
                    for c in forwards[d]:
                        c.wait_recv()
            group = []
            for j in range(1, second_n[d]):
                at_hand = y if d == 0 else x
                t = lax.rem(at_hand + j, second_n[d])
                total = partial(k, d, t, span(k, d), inner(k), slice(None))
                s1[d][j - 1, :, inner(k)] = total.astype(jnp.bfloat16)
                c = pltpu.make_async_remote_copy(
                    src_ref=s1[d].at[j - 1, :, inner(k)], dst_ref=r2[d].at[j - 1, :, inner(k)],
                    send_sem=two_send.at[k, d, j - 1], recv_sem=two_recv.at[k, d, j - 1],
                    device_id=peer_at(1 - d, t, core), device_id_type=MESH,
                )
                c.start()
                group.append(c)
            twos[k, d] = group
        if k < n_sec:
            relay(k + 1)
    for k in range(count, n_sec):
        relay(k + 1)

    def by_block(scalars):
        return jnp.concatenate([jnp.full((block_rows, LANES), s) for s in scalars], axis=0)

    for s in states:
        s.wait()
    layers = [layer_ref[0, b] for b in range(blocks)]
    lives = [valid_ref[0, b] for b in range(blocks)]
    row_decay = by_block([decay_ref[layer] for layer in layers])
    row_live = by_block([jnp.where(v > 0, 1.0, 0.0).astype(jnp.float32) for v in lives]) > 0.5
    for d in range(2):
        for k in range(count):
            if k not in (0, SHIFT):
                pair[k, d].wait_send()

        @pl.when(is_near)
        def _(d=d):
            for c in (kept[0, d], kept[SHIFT, d], *raws[d], *forwards[d], *ones[SHIFT, d], *crosses[d]):
                c.wait_send()

        @pl.when(is_far)
        def _(d=d):
            for c in (pair[0, d], pair[SHIFT, d], *lends[d]):
                c.wait_send()

    zero = jnp.zeros((rows, LANES), jnp.float32)
    sums = (zero, zero)
    for k in range(count):
        for d in range(2):
            with jax.named_scope(f"twow{k}{d}"):
                for c in twos[k, d]:
                    c.wait_recv()

            def update_piece(i, sums, k=k, d=d):
                usum, wsum = sums
                raw_cut = pl.ds(pl.multiple_of(i * LANES, LANES), LANES)
                near_cut = pl.ds(pl.multiple_of(starts[k] + i * LANES, LANES), LANES)
                cut = pl.ds(pl.multiple_of(d * half + starts[k] + i * LANES, LANES), LANES)
                grad = partial(k, d, y if d == 0 else x, cut, near_cut, raw_cut)
                for j in range(second_n[d] - 1):
                    grad += r2[d][j, :, near_cut].astype(jnp.float32)
                weights = p_v[:, cut].astype(jnp.float32)
                old1, old2 = m1_v[:, cut], m2_v[:, cut]
                tenth = 0.1 * grad
                first = 0.9 * old1 + tenth
                second = 0.99 * old2 + tenth * tenth
                root = second * lax.rsqrt(second)
                update = first * (root_second / bias_first) / (root + 1e-06 * root_second) + row_decay * weights
                upd[:, cut] = update
                new1_ref[:, cut] = jnp.where(row_live, first, old1)
                new2_ref[:, cut] = jnp.where(row_live, second, old2)
                return usum + update * update, wsum + weights * weights

            n = (cuts[k] - starts[k]) // LANES
            with jax.named_scope(f"upd{k}{d}"):
                sums = lax.fori_loop(0, n, update_piece, sums, unroll=2 if n % 2 == 0 else (n if n < 4 else 1))

    n_layer = decay_ref.shape[0]
    lane = lax.broadcasted_iota(jnp.int32, (1, LANES), 1)

    def by_layer(values):
        terms = []
        for b in range(blocks):
            chosen = jnp.where(lives[b] > 0, layers[b], -LANES)
            block = values[b * block_rows : (b + 1) * block_rows]
            terms.append(jnp.where(lane == chosen, jnp.sum(block, axis=1, keepdims=True), 0.0))
        return jnp.sum(sum(terms[1:], terms[0]), axis=0, keepdims=True)

    line = (by_layer(sums[1]), by_layer(sums[0]))

    def all_sum(line, slots, send_sem, recv_sem, index, peers):
        for q in range(2):
            slots[index, q] = line[q]
        for peer in peers:
            pltpu.make_async_remote_copy(
                src_ref=slots.at[index], dst_ref=slots.at[index],
                send_sem=send_sem.at[0], recv_sem=recv_sem.at[0],
                device_id=peer, device_id_type=MESH,
            ).start()
        whole = slots.at[pl.ds(0, len(peers))]
        both = pltpu.make_async_remote_copy(
            src_ref=whole, dst_ref=whole, send_sem=send_sem.at[0], recv_sem=recv_sem.at[0],
            device_id=peers[0], device_id_type=MESH,
        )
        with jax.named_scope("allw"):
            both.wait_recv()

        def total(q):
            terms = [slots[j, q] for j in range(len(peers) + 1)]
            while len(terms) > 1:
                terms = [sum(terms[i + 1 : i + 2], terms[i]) for i in range(0, len(terms), 2)]
            return terms[0]

        return (total(0), total(1)), both

    if one_shot:
        every = [
            (i + jnp.where(i >= sec, 1, 0), j) for i in range(n_sec - 1) for j in range(n_shard)
        ] + [(sec, lax.rem(me + j, n_shard)) for j in range(1, n_shard)]
        line, sent = all_sum(line, tiles, t_send, t_recv, sec * n_shard + me, every)
        sends = [sent]
    else:
        shard_peers = [(sec, lax.rem(me + j, n_shard)) for j in range(1, n_shard)]
        sec_peers = [(lax.rem(sec + j, n_sec), me) for j in range(1, n_sec)]
        line, sent = all_sum(line, tiles, t_send, t_recv, me, shard_peers)
        line, zsent = all_sum(line, ztiles, z_send, z_recv, sec, sec_peers)
        sends = [sent, zsent]
    ratios = jnp.sqrt(line[0] / (line[1] + 1.0))
    ratio_ref[...] = ratios[0, :n_layer]
    step_ref[...] = jnp.concatenate(
        [
            jnp.broadcast_to(
                0.1 * jnp.sum(
                    jnp.where((lane == layers[b]) & (lives[b] > 0), ratios, 0.0), axis=1, keepdims=True
                ),
                (block_rows, LANES),
            )
            for b in range(blocks)
        ],
        axis=0,
    )
    with jax.named_scope("endw"):
        for group in (*(ones[k, d] for k in range(count) if k != SHIFT for d in range(2)), *twos.values(), sends):
            for c in group:
                c.wait_send()


def finish(parts, p_v, upd, new1_v, new2_v, step_v, ratio_v, newp_hbm, new1_hbm, new2_hbm, ratio_hbm, newp_v, sem):
    cols = p_v.shape[1]
    width = cols // parts
    copies = [pltpu.make_async_copy(ratio_v, ratio_hbm, sem.at[0])]
    for k in range(parts):
        span = pl.ds(k * width, width)
        for i, (src, dst) in enumerate(((new1_v, new1_hbm), (new2_v, new2_hbm))):
            copies.append(pltpu.make_async_copy(src.at[:, span], dst.at[:, span], sem.at[1 + i * parts + k]))
    for c in copies:
        c.start()
    row_step = step_v[...]

    for k in range(parts):
        def step_piece(i, carry, k=k):
            outer = pl.ds(pl.multiple_of(k * width + i * LANES, LANES), LANES)
            stepped = p_v[:, outer].astype(jnp.float32) - row_step * upd[:, outer]
            newp_v[:, outer] = stepped.astype(jnp.bfloat16)
            return carry

        lax.fori_loop(0, width // LANES, step_piece, 0, unroll=4)
        span = pl.ds(k * width, width)
        c = pltpu.make_async_copy(newp_v.at[:, span], newp_hbm.at[:, span], sem.at[1 + 2 * parts + k])
        c.start()
        copies.append(c)
    for c in copies:
        c.wait()


def shards(grad_parts, params, moment_first, moment_second, block_layer, block_valid, decay):
    n_sec, n_shard = lax.axis_size("section"), lax.axis_size("shard")
    chips = n_shard // 2
    n_y = max(d for d in range(1, math.isqrt(chips) + 1) if chips % d == 0)
    n_x = chips // n_y
    rows, cols = params.shape[1:]
    n_layer = decay.shape[0]
    half = cols // 2
    cuts = tuple(half // LANES * c // CUTS[-1] * LANES for c in CUTS)
    bf16, f32 = jnp.bfloat16, jnp.float32
    dma = pltpu.SemaphoreType.DMA
    one_shot = ONE_SHOT and n_shard * n_sec <= 32
    n_lines = n_shard * n_sec if one_shot else n_shard
    grads = grad_parts.reshape(n_y, n_x, 2, rows, cols)
    any_spec = pl.BlockSpec(memory_space=pltpu.HBM)
    vmem = pl.BlockSpec(memory_space=pltpu.VMEM)
    held = pl.pallas_call(
        functools.partial(kernel, n_sec, n_y, n_x, cuts),
        out_shape=(
            pltpu.VMEM((rows, cols), bf16),
            pltpu.VMEM((rows, cols), f32),
            pltpu.VMEM((rows, cols), f32),
            pltpu.VMEM((rows, cols), f32),
            pltpu.VMEM((rows, LANES), f32),
            pltpu.VMEM((n_layer,), f32),
        ),
        in_specs=[any_spec] * 7,
        out_specs=(vmem,) * 6,
        scratch_shapes=[
            pltpu.VMEM((n_y, n_x, 2, rows, cols), bf16),
            pltpu.VMEM((n_y, n_x, rows, cols), bf16),
            pltpu.VMEM((rows, cols), f32),
            pltpu.VMEM((rows, cols), f32),
            pltpu.VMEM((n_x - 1, n_y, rows, half), bf16),
            pltpu.VMEM((n_y - 1, n_x, rows, half), bf16),
            pltpu.VMEM((n_y - 1, rows, half), bf16),
            pltpu.VMEM((n_x - 1, rows, half), bf16),
            pltpu.VMEM((n_y - 1, rows, half), bf16),
            pltpu.VMEM((n_x - 1, rows, half), bf16),
            pltpu.VMEM((n_x - 1, n_y, rows, cuts[0]), bf16),
            pltpu.VMEM((n_y - 1, n_x, rows, cuts[0]), bf16),
            pltpu.VMEM((n_x - 1, n_y, rows, cuts[SHIFT] - cuts[SHIFT - 1]), bf16),
            pltpu.VMEM((n_y - 1, n_x, rows, cuts[SHIFT] - cuts[SHIFT - 1]), bf16),
            pltpu.VMEM((n_lines, 2, 1, LANES), f32),
            None if one_shot else pltpu.VMEM((n_sec, 2, 1, LANES), f32),
            pltpu.SMEM(block_layer.shape, jnp.int32),
            pltpu.SMEM(block_valid.shape, jnp.int32),
            pltpu.SMEM(decay.shape, f32),
        ],
        compiler_params=pltpu.CompilerParams(
            collective_id=0, has_side_effects=True, vmem_limit_bytes=56 * 1024 * 1024
        ),
    )(grads, params[0], moment_first[0], moment_second[0], block_layer, block_valid, decay)
    out = pl.pallas_call(
        functools.partial(finish, PARTS),
        out_shape=(
            jax.ShapeDtypeStruct((rows, cols), bf16),
            jax.ShapeDtypeStruct((rows, cols), f32),
            jax.ShapeDtypeStruct((rows, cols), f32),
            jax.ShapeDtypeStruct((n_layer,), f32),
        ),
        in_specs=[vmem] * 6,
        out_specs=(any_spec,) * 4,
        scratch_shapes=[pltpu.VMEM((rows, cols), bf16), dma((1 + 3 * PARTS,))],
        compiler_params=pltpu.CompilerParams(vmem_limit_bytes=8 * 1024 * 1024),
    )(*held)
    return (out[0][None], out[1][None], out[2][None], out[3])


def solution(mesh):
    placed = (
        P("section", "shard", None, None),
        P("section", "shard", None),
        P("section", "shard", None),
        P("section", "shard", None),
        P("section", "shard"),
        P("section", "shard"),
        P(),
    )
    return jax.shard_map(
        shards,
        mesh=mesh,
        in_specs=placed,
        out_specs=(
            P("section", "shard", None),
            P("section", "shard", None),
            P("section", "shard", None),
            P(),
        ),
        check_vma=False,
    )
```

```python
import functools
import math

import jax
import jax.numpy as jnp
from jax import lax
from jax.experimental import pallas as pl
from jax.experimental.pallas import tpu as pltpu
from jax.sharding import PartitionSpec as P

MESH = pl.DeviceIdType.MESH
bias_first = 1.0 - 0.9**10
bias_second = 1.0 - 0.99**10
root_second = math.sqrt(bias_second)
LANES = 128
CUTS = (2, 4, 7, 13, 21, 27, 30, 31, 32)
SHIFT = 2
ONE_SHOT = True
PARTS = 2


def kernel(
    n_sec, n_y, n_x, cuts,
    g_hbm, p_hbm, m1_hbm, m2_hbm, layer_hbm, valid_hbm, decay_hbm,
    p_v, upd, new1_ref, new2_ref, step_ref, ratio_ref,
    mine, d2d, m1_v, m2_v, r1x, r1y, s1x, s1y, r2x, r2y, xa, ya, xs, ys, tiles, ztiles, layer_ref, valid_ref, decay_ref,
):
    count = len(cuts)
    most = max(n_x, n_y) - 1
    one_shot = ztiles is None
    dma = pltpu.SemaphoreType.DMA
    pl.run_scoped(
        functools.partial(
            body, n_sec, n_y, n_x, cuts, one_shot,
            g_hbm, p_hbm, m1_hbm, m2_hbm, layer_hbm, valid_hbm, decay_hbm,
            p_v, upd, new1_ref, new2_ref, step_ref, ratio_ref,
            mine, d2d, m1_v, m2_v, (r1x, r1y), (s1x, s1y), (r2x, r2y), (xa, ya), (xs, ys), tiles, ztiles,
            layer_ref, valid_ref, decay_ref,
        ),
        load_sem=dma((count, 2)),
        state_sem=dma((6,)),
        pair_send=dma((count, 2)),
        one_send=dma((count, 2, most)),
        two_send=dma((count, 2, most)),
        raw_send=dma((2, 2, most)),
        lent_send=dma((2, 2, most)),
        lent_recv=dma((2, most)),
        t_send=dma((1,)),
        z_send=dma((1,)),
        pair_recv=dma((count, 2)),
        one_recv=dma((count, 2, most)),
        two_recv=dma((count, 2, most)),
        raw_recv=dma((2, most)),
        t_recv=dma((1,)),
        z_recv=dma((1,)),
        told=pltpu.SemaphoreType.REGULAR((2, n_sec - 1)),
        inside=pltpu.SemaphoreType.REGULAR,
    )


def body(
    n_sec, n_y, n_x, cuts, one_shot,
    g_hbm, p_hbm, m1_hbm, m2_hbm, layer_hbm, valid_hbm, decay_hbm,
    p_v, upd, new1_ref, new2_ref, step_ref, ratio_ref,
    mine, d2d, m1_v, m2_v, r1, s1, r2, other, lent, tiles, ztiles, layer_ref, valid_ref, decay_ref,
    load_sem, state_sem, pair_send, one_send, two_send, raw_send, lent_send, lent_recv, t_send, z_send,
    pair_recv, one_recv, two_recv, raw_recv, t_recv, z_recv, told, inside,
):
    rows, cols = p_v.shape
    half = cols // 2
    count = len(cuts)
    n_shard = 2 * n_y * n_x
    sec, me = lax.axis_index("section"), lax.axis_index("shard")
    core = lax.rem(me, 2)
    is_far, is_near = core == 0, core == 1
    x = lax.rem(me // 2, n_x)
    y = me // (2 * n_x)
    blocks = layer_ref.shape[1]
    block_rows = rows // blocks

    def at(yy, xx, cc):
        return (sec, (yy * n_x + xx) * 2 + cc)

    starts = (0,) + cuts[:-1]

    def span(k, d):
        return pl.ds(d * half + starts[k], cuts[k] - starts[k])

    def inner(k):
        return pl.ds(starts[k], cuts[k] - starts[k])

    loads = {}
    for k in range(count):
        for d in range(2):
            c = pltpu.make_async_copy(
                g_hbm.at[:, :, :, :, span(k, d)], mine.at[:, :, :, :, span(k, d)], load_sem.at[k, d]
            )
            c.start()
            loads[k, d] = c
        if k == 0:
            barrier = pltpu.get_barrier_semaphore()
            beside = at(y, x, 1 - core)
            around = [at(y, lax.rem(x + j, n_x), 1) for j in range(1, n_x)]
            around += [at(lax.rem(y + j, n_y), x, 1) for j in range(1, n_y)]
            for peer in around:
                pl.semaphore_signal(barrier, inc=1, device_id=peer, device_id_type=MESH)
            last_sec = n_sec - 1
            up = (jnp.minimum(sec + 1, last_sec), me)
            down = (jnp.maximum(sec - 1, 0), me)

            @pl.when(sec < last_sec)
            def _():
                pl.semaphore_signal(barrier, inc=1, device_id=(up[0], me - core + 1), device_id_type=MESH)

            @pl.when(sec > 0)
            def _():
                pl.semaphore_signal(barrier, inc=1, device_id=(down[0], me - core + 1), device_id_type=MESH)

            @pl.when(is_near)
            def _():
                pl.semaphore_signal(barrier, inc=1, device_id=beside, device_id_type=MESH)

    states = [
        pltpu.make_async_copy(src, dst, state_sem.at[i])
        for i, (src, dst) in enumerate(
            (
                (layer_hbm, layer_ref), (valid_hbm, valid_ref), (decay_hbm, decay_ref),
                (p_hbm, p_v), (m1_hbm, m1_v), (m2_hbm, m2_v),
            )
        )
    ]
    for s in states:
        s.start()

    ends = jnp.where(sec < last_sec, 1, 0) + jnp.where(sec > 0, 1, 0)

    @pl.when(is_far)
    def _():
        pl.semaphore_wait(barrier, 1)
        pl.semaphore_signal(inside, inc=1, device_id=beside, device_id_type=MESH)

    @pl.when(is_near)
    def _():
        pl.semaphore_wait(inside, 1)

    def meet():
        with jax.named_scope("bar"):

            @pl.when(is_near)
            def _():
                pl.semaphore_wait(barrier, 2 * (len(around) + ends))
                pl.semaphore_signal(inside, inc=1, device_id=beside, device_id_type=MESH)

            @pl.when(is_far)
            def _():
                pl.semaphore_wait(inside, 1)

    def relay(d):
        if 1 < d <= n_sec:

            @pl.when(sec >= d - 1)
            def _():
                pl.semaphore_wait(told.at[0, d - 2], 1)

            @pl.when(sec <= n_sec - d)
            def _():
                pl.semaphore_wait(told.at[1, d - 2], 1)

        if d < n_sec:

            @pl.when((sec >= d - 1) & (sec < last_sec))
            def _():
                pl.semaphore_signal(told.at[0, d - 1], inc=1, device_id=up, device_id_type=MESH)

            @pl.when((sec <= n_sec - d) & (sec > 0))
            def _():
                pl.semaphore_signal(told.at[1, d - 1], inc=1, device_id=down, device_id_type=MESH)

    def place(d, t):
        return (slice(None), t) if d == 0 else (t, slice(None))

    def peer_at(d, t, cc):
        return at(y, t, cc) if d == 0 else at(t, x, cc)

    here = (x, y)
    first_n, second_n = (n_x, n_y), (n_y, n_x)

    def others(d):
        return [(j, lax.rem(here[d] + j, first_n[d])) for j in range(1, first_n[d])]

    def remote(src, dst, send_sem, recv_sem, peer):
        return pltpu.make_async_remote_copy(
            src_ref=src, dst_ref=dst, send_sem=send_sem, recv_sem=recv_sem, device_id=peer, device_id_type=MESH
        )

    def rows_of(d, t, cc, k):
        return mine.at[(*place(d, t), cc, slice(None), span(k, d))]

    ones, raws, forwards, lends, crosses, pair, kept = {}, {}, {}, {}, {}, {}, {}
    for d in range(2):
        for k in range(count):
            ones[k, d] = [
                remote(
                    rows_of(d, t, core, k), r1[d].at[j - 1, :, :, inner(k)],
                    one_send.at[k, d, j - 1], one_recv.at[k, d, j - 1], peer_at(d, t, core),
                )
                for j, t in others(d)
            ]
            for group, t in ((pair, slice(None)), (kept, here[d])):
                if group is kept and k not in (0, SHIFT):
                    continue
                spot = place(d, t)
                group[k, d] = remote(
                    rows_of(d, t, 1 - core, k), d2d.at[(*spot, slice(None), span(k, d))],
                    pair_send.at[k, d], pair_recv.at[k, d], at(y, x, 1 - core),
                )
        raws[d] = [
            remote(
                rows_of(d, t, 1 - core, 0), other[d].at[j - 1],
                raw_send.at[0, d, j - 1], raw_recv.at[d, j - 1], peer_at(d, t, 1 - core),
            )
            for j, t in others(d)
        ]
        forwards[d] = [
            remote(
                d2d.at[(*place(d, t), slice(None), span(0, d))], other[d].at[j - 1],
                raw_send.at[1, d, j - 1], raw_recv.at[d, j - 1], peer_at(d, t, core),
            )
            for j, t in others(d)
        ]
        lends[d] = [
            remote(
                rows_of(d, t, core, SHIFT), lent[d].at[j - 1],
                lent_send.at[0, d, j - 1], lent_recv.at[d, j - 1], at(y, x, 1 - core),
            )
            for j, t in others(d)
        ]
        crosses[d] = [
            remote(
                rows_of(d, t, 1 - core, SHIFT), r1[d].at[j - 1, :, :, inner(SHIFT)],
                lent_send.at[1, d, j - 1], one_recv.at[SHIFT, d, j - 1], peer_at(d, t, 1 - core),
            )
            for j, t in others(d)
        ]

    def send_raw(d):
        for c in ones[0, d]:
            c.start()

        @pl.when(is_near)
        def _():
            for c in raws[d]:
                c.start()

    def send_pair(k, d):
        with jax.named_scope(f"ldw{k}{d}"):
            loads[k, d].wait()
        if k in (0, SHIFT):

            @pl.when(is_far)
            def _():
                pair[k, d].start()
                if k:
                    for c in lends[d]:
                        c.start()

            @pl.when(is_near)
            def _():
                kept[k, d].start()
        else:
            pair[k, d].start()

    def add_pair(yy, xx, cut):
        total = mine[yy, xx, core, :, cut].astype(jnp.float32) + d2d[yy, xx, :, cut].astype(jnp.float32)
        mine[yy, xx, core, :, cut] = total.astype(jnp.bfloat16)

    def add_all(cut):
        def add_one(i, carry):
            add_pair(i // n_x, lax.rem(i, n_x), cut)
            return carry

        lax.fori_loop(0, n_y * n_x, add_one, 0)

    def add_kept(d, cut):
        for i in range(second_n[d]):
            add_pair(i if d == 0 else y, x if d == 0 else i, cut)

    def send_one(k, d):
        cut = span(k, d)
        if k == 0:

            @pl.when(is_near)
            def _():
                pair[k, d].wait_recv()
                for c in forwards[d]:
                    c.start()

            @pl.when(is_far)
            def _():
                kept[k, d].wait_recv()

            add_kept(d, cut)
        elif k == SHIFT:

            @pl.when(is_near)
            def _():
                pair[k, d].wait_recv()
                for c in lends[d]:
                    c.wait_recv()
                add_all(cut)
                for c in ones[k, d]:
                    c.start()
                for j, t in others(d):
                    for i in range(second_n[d]):
                        yy, xx = (i, t) if d == 0 else (t, i)
                        total = mine[yy, xx, 1 - core, :, cut].astype(jnp.float32)
                        total += lent[d][j - 1, i].astype(jnp.float32)
                        mine[yy, xx, 1 - core, :, cut] = total.astype(jnp.bfloat16)
                for c in crosses[d]:
                    c.start()

            @pl.when(is_far)
            def _():
                kept[k, d].wait_recv()
                add_kept(d, cut)
        else:
            with jax.named_scope(f"pairw{k}{d}"):
                pair[k, d].wait_recv()
            add_all(cut)
            for c in ones[k, d]:
                c.start()

    ahead = 3
    order = [1, 0, *range(2, count)]
    for i, k in enumerate(order[: 1 + ahead]):
        if i == 2:
            meet()
            for d in range(2):
                send_raw(d)
        for d in range(2):
            send_pair(k, d)
    for i, k in enumerate(order):
        for d in range(2):
            send_one(k, d)
        if i + 1 + ahead < count:
            for d in range(2):
                send_pair(order[i + 1 + ahead], d)

    def partial(k, d, t, cut, near_cut, raw_cut):
        yy, xx = (t, x) if d == 0 else (y, t)
        total = mine[yy, xx, core, :, cut].astype(jnp.float32)
        for i in range(first_n[d] - 1):
            total += r1[d][i, t, :, near_cut].astype(jnp.float32)
            if k == 0:
                total += other[d][i, t, :, raw_cut].astype(jnp.float32)
        return total

    def by_block(scalars):
        return jnp.concatenate([jnp.full((block_rows, LANES), s) for s in scalars], axis=0)

    for s in states:
        s.wait()
    layers = [layer_ref[0, b] for b in range(blocks)]
    lives = [valid_ref[0, b] for b in range(blocks)]
    row_decay = by_block([decay_ref[layer] for layer in layers])
    row_live = by_block([jnp.where(v > 0, 1.0, 0.0).astype(jnp.float32) for v in lives]) > 0.5
    n_layer = decay_ref.shape[0]
    lane = lax.broadcasted_iota(jnp.int32, (1, LANES), 1)

    def by_layer(values, offset):
        terms = []
        for b in range(blocks):
            chosen = jnp.where(lives[b] > 0, layers[b] + offset, -1)
            block = values[b * block_rows : (b + 1) * block_rows]
            terms.append(jnp.where(lane == chosen, jnp.sum(block, axis=1, keepdims=True), 0.0))
        return jnp.sum(sum(terms[1:], terms[0]), axis=0, keepdims=True)

    def weigh(i, wsum):
        weights = p_v[:, pl.ds(pl.multiple_of(i * LANES, LANES), LANES)].astype(jnp.float32)
        return wsum + weights * weights

    zero = jnp.zeros((rows, LANES), jnp.float32)
    weight_line = by_layer(lax.fori_loop(0, cols // LANES, weigh, zero, unroll=2), 0)

    twos = {}
    for k in range(count):
        for d in range(2):
            with jax.named_scope(f"onew{k}{d}"):
                for c in ones[k, d]:
                    c.wait_recv()
                if k == 0:
                    for c in forwards[d]:
                        c.wait_recv()
            group = []
            for j in range(1, second_n[d]):
                at_hand = y if d == 0 else x
                t = lax.rem(at_hand + j, second_n[d])
                total = partial(k, d, t, span(k, d), inner(k), slice(None))
                s1[d][j - 1, :, inner(k)] = total.astype(jnp.bfloat16)
                c = pltpu.make_async_remote_copy(
                    src_ref=s1[d].at[j - 1, :, inner(k)], dst_ref=r2[d].at[j - 1, :, inner(k)],
                    send_sem=two_send.at[k, d, j - 1], recv_sem=two_recv.at[k, d, j - 1],
                    device_id=peer_at(1 - d, t, core), device_id_type=MESH,
                )
                c.start()
                group.append(c)
            twos[k, d] = group
        if k < n_sec:
            relay(k + 1)
    for k in range(count, n_sec):
        relay(k + 1)

    for d in range(2):
        for k in range(count):
            if k not in (0, SHIFT):
                pair[k, d].wait_send()

        @pl.when(is_near)
        def _(d=d):
            for c in (kept[0, d], kept[SHIFT, d], *raws[d], *forwards[d], *ones[SHIFT, d], *crosses[d]):
                c.wait_send()

        @pl.when(is_far)
        def _(d=d):
            for c in (pair[0, d], pair[SHIFT, d], *lends[d]):
                c.wait_send()

    usum = zero
    for k in range(count):
        for d in range(2):
            with jax.named_scope(f"twow{k}{d}"):
                for c in twos[k, d]:
                    c.wait_recv()

            def update_piece(i, usum, k=k, d=d):
                raw_cut = pl.ds(pl.multiple_of(i * LANES, LANES), LANES)
                near_cut = pl.ds(pl.multiple_of(starts[k] + i * LANES, LANES), LANES)
                cut = pl.ds(pl.multiple_of(d * half + starts[k] + i * LANES, LANES), LANES)
                grad = partial(k, d, y if d == 0 else x, cut, near_cut, raw_cut)
                for j in range(second_n[d] - 1):
                    grad += r2[d][j, :, near_cut].astype(jnp.float32)
                weights = p_v[:, cut].astype(jnp.float32)
                old1, old2 = m1_v[:, cut], m2_v[:, cut]
                tenth = 0.1 * grad
                first = 0.9 * old1 + tenth
                second = 0.99 * old2 + tenth * tenth
                root = second * lax.rsqrt(second)
                update = first * (root_second / bias_first) / (root + 1e-06 * root_second) + row_decay * weights
                upd[:, cut] = update
                new1_ref[:, cut] = jnp.where(row_live, first, old1)
                new2_ref[:, cut] = jnp.where(row_live, second, old2)
                return usum + update * update

            n = (cuts[k] - starts[k]) // LANES
            with jax.named_scope(f"upd{k}{d}"):
                usum = lax.fori_loop(0, n, update_piece, usum, unroll=2 if n % 2 == 0 else (n if n < 4 else 1))

    line = weight_line + by_layer(usum, n_layer)

    def all_sum(line, slots, send_sem, recv_sem, index, peers, sent):
        slots[index] = line
        for peer in peers:
            pltpu.make_async_remote_copy(
                src_ref=slots.at[index], dst_ref=slots.at[index],
                send_sem=send_sem.at[0], recv_sem=recv_sem.at[0],
                device_id=peer, device_id_type=MESH,
            ).start()
        whole = slots.at[pl.ds(0, len(peers))]
        both = pltpu.make_async_remote_copy(
            src_ref=whole, dst_ref=whole, send_sem=send_sem.at[0], recv_sem=recv_sem.at[0],
            device_id=peers[0], device_id_type=MESH,
        )
        if sent:
            with jax.named_scope("endw"):
                for c in sent:
                    c.wait_send()
        with jax.named_scope("allw"):
            both.wait_recv()
        terms = [slots[j] for j in range(len(peers) + 1)]
        while len(terms) > 1:
            terms = [sum(terms[i + 1 : i + 2], terms[i]) for i in range(0, len(terms), 2)]
        return terms[0], both

    groups = (*(ones[k, d] for k in range(count) if k != SHIFT for d in range(2)), *twos.values())
    sent = [c for group in groups for c in group]
    if one_shot:
        every = [
            (i + jnp.where(i >= sec, 1, 0), j) for i in range(n_sec - 1) for j in range(n_shard)
        ] + [(sec, lax.rem(me + j, n_shard)) for j in range(1, n_shard)]
        line, last = all_sum(line, tiles, t_send, t_recv, sec * n_shard + me, every, sent)
        sends = [last]
    else:
        shard_peers = [(sec, lax.rem(me + j, n_shard)) for j in range(1, n_shard)]
        sec_peers = [(lax.rem(sec + j, n_sec), me) for j in range(1, n_sec)]
        line, last = all_sum(line, tiles, t_send, t_recv, me, shard_peers, sent)
        line, zlast = all_sum(line, ztiles, z_send, z_recv, sec, sec_peers, [])
        sends = [last, zlast]
    ratios = jnp.sqrt(line / (pltpu.roll(line, LANES - n_layer, 1) + 1.0))
    ratio_ref[...] = ratios[0, :n_layer]
    step_ref[...] = jnp.concatenate(
        [
            jnp.broadcast_to(
                0.1 * jnp.sum(
                    jnp.where((lane == layers[b]) & (lives[b] > 0), ratios, 0.0), axis=1, keepdims=True
                ),
                (block_rows, LANES),
            )
            for b in range(blocks)
        ],
        axis=0,
    )
    for c in sends:
        c.wait_send()


def finish(parts, p_v, upd, new1_v, new2_v, step_v, ratio_v, newp_hbm, new1_hbm, new2_hbm, ratio_hbm, newp_v, sem):
    cols = p_v.shape[1]
    width = cols // parts
    copies = [pltpu.make_async_copy(ratio_v, ratio_hbm, sem.at[0])]
    for k in range(parts):
        span = pl.ds(k * width, width)
        for i, (src, dst) in enumerate(((new1_v, new1_hbm), (new2_v, new2_hbm))):
            copies.append(pltpu.make_async_copy(src.at[:, span], dst.at[:, span], sem.at[1 + i * parts + k]))
    for c in copies:
        c.start()
    row_step = step_v[...]

    for k in range(parts):
        def step_piece(i, carry, k=k):
            outer = pl.ds(pl.multiple_of(k * width + i * LANES, LANES), LANES)
            stepped = p_v[:, outer].astype(jnp.float32) - row_step * upd[:, outer]
            newp_v[:, outer] = stepped.astype(jnp.bfloat16)
            return carry

        lax.fori_loop(0, width // LANES, step_piece, 0, unroll=4)
        span = pl.ds(k * width, width)
        c = pltpu.make_async_copy(newp_v.at[:, span], newp_hbm.at[:, span], sem.at[1 + 2 * parts + k])
        c.start()
        copies.append(c)
    for c in copies:
        c.wait()


def shards(grad_parts, params, moment_first, moment_second, block_layer, block_valid, decay):
    n_sec, n_shard = lax.axis_size("section"), lax.axis_size("shard")
    chips = n_shard // 2
    n_y = max(d for d in range(1, math.isqrt(chips) + 1) if chips % d == 0)
    n_x = chips // n_y
    rows, cols = params.shape[1:]
    n_layer = decay.shape[0]
    half = cols // 2
    cuts = tuple(half // LANES * c // CUTS[-1] * LANES for c in CUTS)
    bf16, f32 = jnp.bfloat16, jnp.float32
    dma = pltpu.SemaphoreType.DMA
    one_shot = ONE_SHOT and n_shard * n_sec <= 32
    n_lines = n_shard * n_sec if one_shot else n_shard
    grads = grad_parts.reshape(n_y, n_x, 2, rows, cols)
    any_spec = pl.BlockSpec(memory_space=pltpu.HBM)
    vmem = pl.BlockSpec(memory_space=pltpu.VMEM)
    held = pl.pallas_call(
        functools.partial(kernel, n_sec, n_y, n_x, cuts),
        out_shape=(
            pltpu.VMEM((rows, cols), bf16),
            pltpu.VMEM((rows, cols), f32),
            pltpu.VMEM((rows, cols), f32),
            pltpu.VMEM((rows, cols), f32),
            pltpu.VMEM((rows, LANES), f32),
            pltpu.VMEM((n_layer,), f32),
        ),
        in_specs=[any_spec] * 7,
        out_specs=(vmem,) * 6,
        scratch_shapes=[
            pltpu.VMEM((n_y, n_x, 2, rows, cols), bf16),
            pltpu.VMEM((n_y, n_x, rows, cols), bf16),
            pltpu.VMEM((rows, cols), f32),
            pltpu.VMEM((rows, cols), f32),
            pltpu.VMEM((n_x - 1, n_y, rows, half), bf16),
            pltpu.VMEM((n_y - 1, n_x, rows, half), bf16),
            pltpu.VMEM((n_y - 1, rows, half), bf16),
            pltpu.VMEM((n_x - 1, rows, half), bf16),
            pltpu.VMEM((n_y - 1, rows, half), bf16),
            pltpu.VMEM((n_x - 1, rows, half), bf16),
            pltpu.VMEM((n_x - 1, n_y, rows, cuts[0]), bf16),
            pltpu.VMEM((n_y - 1, n_x, rows, cuts[0]), bf16),
            pltpu.VMEM((n_x - 1, n_y, rows, cuts[SHIFT] - cuts[SHIFT - 1]), bf16),
            pltpu.VMEM((n_y - 1, n_x, rows, cuts[SHIFT] - cuts[SHIFT - 1]), bf16),
            pltpu.VMEM((n_lines, 1, LANES), f32),
            None if one_shot else pltpu.VMEM((n_sec, 1, LANES), f32),
            pltpu.SMEM(block_layer.shape, jnp.int32),
            pltpu.SMEM(block_valid.shape, jnp.int32),
            pltpu.SMEM(decay.shape, f32),
        ],
        compiler_params=pltpu.CompilerParams(
            collective_id=0, has_side_effects=True, vmem_limit_bytes=56 * 1024 * 1024
        ),
    )(grads, params[0], moment_first[0], moment_second[0], block_layer, block_valid, decay)
    out = pl.pallas_call(
        functools.partial(finish, PARTS),
        out_shape=(
            jax.ShapeDtypeStruct((rows, cols), bf16),
            jax.ShapeDtypeStruct((rows, cols), f32),
            jax.ShapeDtypeStruct((rows, cols), f32),
            jax.ShapeDtypeStruct((n_layer,), f32),
        ),
        in_specs=[vmem] * 6,
        out_specs=(any_spec,) * 4,
        scratch_shapes=[pltpu.VMEM((rows, cols), bf16), dma((1 + 3 * PARTS,))],
        compiler_params=pltpu.CompilerParams(vmem_limit_bytes=8 * 1024 * 1024),
    )(*held)
    return (out[0][None], out[1][None], out[2][None], out[3])


def solution(mesh):
    placed = (
        P("section", "shard", None, None),
        P("section", "shard", None),
        P("section", "shard", None),
        P("section", "shard", None),
        P("section", "shard"),
        P("section", "shard"),
        P(),
    )
    return jax.shard_map(
        shards,
        mesh=mesh,
        in_specs=placed,
        out_specs=(
            P("section", "shard", None),
            P("section", "shard", None),
            P("section", "shard", None),
            P(),
        ),
        check_vma=False,
    )
```

```python
import functools
import math

import jax
import jax.numpy as jnp
from jax import lax
from jax.experimental import pallas as pl
from jax.experimental.pallas import tpu as pltpu
from jax.sharding import PartitionSpec as P

MESH = pl.DeviceIdType.MESH
bias_first = 1.0 - 0.9**10
bias_second = 1.0 - 0.99**10
root_second = math.sqrt(bias_second)
LANES = 128
CUTS = (3, 5, 9, 17, 24, 28, 31, 32)
SHIFT = 2
ONE_SHOT = True
PARTS = 2
WIDE = 4


def kernel(
    n_sec, n_y, n_x, cuts,
    g_hbm, p_hbm, m1_hbm, m2_hbm, layer_hbm, valid_hbm, decay_hbm,
    p_v, upd, new1_ref, new2_ref, step_ref, ratio_ref,
    mine, d2d, m1_v, m2_v, r1x, r1y, s1x, s1y, r2x, r2y, xa, ya, xs, ys, tiles, ztiles, layer_ref, valid_ref, decay_ref,
):
    count = len(cuts)
    most = max(n_x, n_y) - 1
    one_shot = ztiles is None
    dma = pltpu.SemaphoreType.DMA
    pl.run_scoped(
        functools.partial(
            body, n_sec, n_y, n_x, cuts, one_shot,
            g_hbm, p_hbm, m1_hbm, m2_hbm, layer_hbm, valid_hbm, decay_hbm,
            p_v, upd, new1_ref, new2_ref, step_ref, ratio_ref,
            mine, d2d, m1_v, m2_v, (r1x, r1y), (s1x, s1y), (r2x, r2y), (xa, ya), (xs, ys), tiles, ztiles,
            layer_ref, valid_ref, decay_ref,
        ),
        load_sem=dma((count, 2)),
        state_sem=dma((6,)),
        pair_send=dma((count, 2)),
        one_send=dma((count, 2, most)),
        two_send=dma((count, 2, most)),
        raw_send=dma((2, most)),
        lent_send=dma((2, 2, most)),
        lent_recv=dma((2, most)),
        t_send=dma((1,)),
        z_send=dma((1,)),
        pair_recv=dma((count, 2)),
        one_recv=dma((count, 2, most)),
        two_recv=dma((count, 2, most)),
        raw_recv=dma((2, most)),
        t_recv=dma((1,)),
        z_recv=dma((1,)),
        told=pltpu.SemaphoreType.REGULAR((2, n_sec - 1)),
        inside=pltpu.SemaphoreType.REGULAR,
        whole=pltpu.SemaphoreType.REGULAR,
        settled=pltpu.SemaphoreType.REGULAR,
    )


def body(
    n_sec, n_y, n_x, cuts, one_shot,
    g_hbm, p_hbm, m1_hbm, m2_hbm, layer_hbm, valid_hbm, decay_hbm,
    p_v, upd, new1_ref, new2_ref, step_ref, ratio_ref,
    mine, d2d, m1_v, m2_v, r1, s1, r2, other, lent, tiles, ztiles, layer_ref, valid_ref, decay_ref,
    load_sem, state_sem, pair_send, one_send, two_send, raw_send, lent_send, lent_recv, t_send, z_send,
    pair_recv, one_recv, two_recv, raw_recv, t_recv, z_recv, told, inside, whole, settled,
):
    rows, cols = p_v.shape
    half = cols // 2
    count = len(cuts)
    n_shard = 2 * n_y * n_x
    sec, me = lax.axis_index("section"), lax.axis_index("shard")
    core = lax.rem(me, 2)
    is_far, is_near = core == 0, core == 1
    x = lax.rem(me // 2, n_x)
    y = me // (2 * n_x)
    blocks = layer_ref.shape[1]
    block_rows = rows // blocks

    def at(yy, xx, cc):
        return (sec, (yy * n_x + xx) * 2 + cc)

    starts = (0,) + cuts[:-1]

    def span(k, d):
        return pl.ds(d * half + starts[k], cuts[k] - starts[k])

    def inner(k):
        return pl.ds(starts[k], cuts[k] - starts[k])

    loads = {}
    for k in range(count):
        for d in range(2):
            c = pltpu.make_async_copy(
                g_hbm.at[:, :, :, :, span(k, d)], mine.at[:, :, :, :, span(k, d)], load_sem.at[k, d]
            )
            c.start()
            loads[k, d] = c
        if k == 0:
            barrier = pltpu.get_barrier_semaphore()
            beside = at(y, x, 1 - core)
            around = [at(y, lax.rem(x + j, n_x), core) for j in range(1, n_x)]
            around += [at(lax.rem(y + j, n_y), x, core) for j in range(1, n_y)]
            last_sec = n_sec - 1
            up = (jnp.minimum(sec + 1, last_sec), me)
            down = (jnp.maximum(sec - 1, 0), me)
            ends = jnp.where(sec < last_sec, 1, 0) + jnp.where(sec > 0, 1, 0)

            def tell(semaphore):
                for peer in around:
                    pl.semaphore_signal(semaphore, inc=1, device_id=peer, device_id_type=MESH)

                @pl.when(sec < last_sec)
                def _():
                    pl.semaphore_signal(semaphore, inc=1, device_id=up, device_id_type=MESH)

                @pl.when(sec > 0)
                def _():
                    pl.semaphore_signal(semaphore, inc=1, device_id=down, device_id_type=MESH)

            @pl.when(is_near)
            def _():
                tell(barrier)
                pl.semaphore_signal(barrier, inc=1, device_id=beside, device_id_type=MESH)

    states = [
        pltpu.make_async_copy(src, dst, state_sem.at[i])
        for i, (src, dst) in enumerate(
            (
                (layer_hbm, layer_ref), (valid_hbm, valid_ref), (decay_hbm, decay_ref),
                (p_hbm, p_v), (m1_hbm, m1_v), (m2_hbm, m2_v),
            )
        )
    ]
    for s in states:
        s.start()

    @pl.when(is_far)
    def _():
        pl.semaphore_wait(barrier, 1)
        pl.semaphore_signal(inside, inc=1, device_id=beside, device_id_type=MESH)
        for d in range(2):
            other[d][...] = jnp.zeros_like(other[d])

    @pl.when(is_near)
    def _():
        with jax.named_scope("bar1"):
            pl.semaphore_wait(inside, 1)
            pl.semaphore_wait(barrier, len(around) + ends)
        tell(whole)
        pl.semaphore_signal(inside, inc=1, device_id=beside, device_id_type=MESH)

    def meet():
        with jax.named_scope("bar"):

            @pl.when(is_near)
            def _():
                pl.semaphore_wait(whole, len(around) + ends)
                pl.semaphore_signal(settled, inc=1, device_id=beside, device_id_type=MESH)

            @pl.when(is_far)
            def _():
                pl.semaphore_wait(settled, 1)

    def relay(d):
        if 1 < d <= n_sec:

            @pl.when(sec >= d - 1)
            def _():
                pl.semaphore_wait(told.at[0, d - 2], 1)

            @pl.when(sec <= n_sec - d)
            def _():
                pl.semaphore_wait(told.at[1, d - 2], 1)

        if d < n_sec:

            @pl.when((sec >= d - 1) & (sec < last_sec))
            def _():
                pl.semaphore_signal(told.at[0, d - 1], inc=1, device_id=up, device_id_type=MESH)

            @pl.when((sec <= n_sec - d) & (sec > 0))
            def _():
                pl.semaphore_signal(told.at[1, d - 1], inc=1, device_id=down, device_id_type=MESH)

    def place(d, t):
        return (slice(None), t) if d == 0 else (t, slice(None))

    def peer_at(d, t, cc):
        return at(y, t, cc) if d == 0 else at(t, x, cc)

    here = (x, y)
    first_n, second_n = (n_x, n_y), (n_y, n_x)

    def others(d):
        return [(j, lax.rem(here[d] + j, first_n[d])) for j in range(1, first_n[d])]

    def remote(src, dst, send_sem, recv_sem, peer):
        return pltpu.make_async_remote_copy(
            src_ref=src, dst_ref=dst, send_sem=send_sem, recv_sem=recv_sem, device_id=peer, device_id_type=MESH
        )

    def rows_of(d, t, cc, k):
        return mine.at[(*place(d, t), cc, slice(None), span(k, d))]

    ones, raws, lends, crosses, pair, kept = {}, {}, {}, {}, {}, {}
    for d in range(2):
        for k in range(count):
            ones[k, d] = [
                remote(
                    rows_of(d, t, core, k), r1[d].at[j - 1, :, :, inner(k)],
                    one_send.at[k, d, j - 1], one_recv.at[k, d, j - 1], peer_at(d, t, core),
                )
                for j, t in others(d)
            ]
            for group, t in ((pair, slice(None)), (kept, here[d])):
                if group is kept and k not in (0, SHIFT):
                    continue
                spot = place(d, t)
                group[k, d] = remote(
                    rows_of(d, t, 1 - core, k), d2d.at[(*spot, slice(None), span(k, d))],
                    pair_send.at[k, d], pair_recv.at[k, d], at(y, x, 1 - core),
                )
        raws[d] = [
            remote(
                rows_of(d, t, 1 - core, 0), other[d].at[j - 1],
                raw_send.at[d, j - 1], raw_recv.at[d, j - 1], peer_at(d, t, 1 - core),
            )
            for j, t in others(d)
        ]
        lends[d] = [
            remote(
                rows_of(d, t, core, SHIFT), lent[d].at[j - 1],
                lent_send.at[0, d, j - 1], lent_recv.at[d, j - 1], at(y, x, 1 - core),
            )
            for j, t in others(d)
        ]
        crosses[d] = [
            remote(
                rows_of(d, t, 1 - core, SHIFT), r1[d].at[j - 1, :, :, inner(SHIFT)],
                lent_send.at[1, d, j - 1], one_recv.at[SHIFT, d, j - 1], peer_at(d, t, 1 - core),
            )
            for j, t in others(d)
        ]

    def send_pair(k, d):
        if k:
            with jax.named_scope(f"ldw{k}{d}"):
                loads[k, d].wait()
        if k == 0:

            @pl.when(is_far)
            def _():
                kept[k, d].start()

            @pl.when(is_near)
            def _():
                pair[k, d].start()
        elif k == SHIFT:

            @pl.when(is_far)
            def _():
                for c in (pair[k, d], *lends[d]):
                    c.start()

            @pl.when(is_near)
            def _():
                kept[k, d].start()
        else:
            pair[k, d].start()

    def add_pair(yy, xx, cut):
        total = mine[yy, xx, core, :, cut].astype(jnp.float32) + d2d[yy, xx, :, cut].astype(jnp.float32)
        mine[yy, xx, core, :, cut] = total.astype(jnp.bfloat16)

    def add_all(cut):
        def add_one(i, carry):
            add_pair(i // n_x, lax.rem(i, n_x), cut)
            return carry

        lax.fori_loop(0, n_y * n_x, add_one, 0)

    def add_kept(d, cut):
        for i in range(second_n[d]):
            add_pair(i if d == 0 else y, x if d == 0 else i, cut)

    def send_one(k, d):
        cut = span(k, d)
        if k == 0:

            @pl.when(is_near)
            def _():
                kept[k, d].wait_recv()
                add_kept(d, cut)

            @pl.when(is_far)
            def _():
                pair[k, d].wait_recv()
                add_all(cut)
                for c in ones[k, d]:
                    c.start()

        elif k == SHIFT:

            @pl.when(is_near)
            def _():
                pair[k, d].wait_recv()
                for c in lends[d]:
                    c.wait_recv()
                add_all(cut)
                for c in ones[k, d]:
                    c.start()
                for j, t in others(d):
                    for i in range(second_n[d]):
                        yy, xx = (i, t) if d == 0 else (t, i)
                        total = mine[yy, xx, 1 - core, :, cut].astype(jnp.float32)
                        total += lent[d][j - 1, i].astype(jnp.float32)
                        mine[yy, xx, 1 - core, :, cut] = total.astype(jnp.bfloat16)
                for c in crosses[d]:
                    c.start()

            @pl.when(is_far)
            def _():
                kept[k, d].wait_recv()
                add_kept(d, cut)
        else:
            with jax.named_scope(f"pairw{k}{d}"):
                pair[k, d].wait_recv()
            add_all(cut)
            for c in ones[k, d]:
                c.start()

    for d in range(2):
        with jax.named_scope(f"ldw0{d}"):
            loads[0, d].wait()

        @pl.when(is_near)
        def _(d=d):
            for c in ones[0, d]:
                c.start()

    ahead = 3
    order = [1, 0, *range(2, count)]
    for i, k in enumerate(order[: 1 + ahead]):
        if i == 2:

            @pl.when(is_far)
            def _():
                pl.semaphore_wait(inside, 1)
                for d in range(2):
                    for c in raws[d]:
                        c.start()

            meet()
        for d in range(2):
            send_pair(k, d)
    for i, k in enumerate(order):
        for d in range(2):
            send_one(k, d)
        if i + 1 + ahead < count:
            for d in range(2):
                send_pair(order[i + 1 + ahead], d)

    def partial(k, d, t, cut, near_cut, raw_cut):
        yy, xx = (t, x) if d == 0 else (y, t)
        total = mine[yy, xx, core, :, cut].astype(jnp.float32)
        for i in range(first_n[d] - 1):
            total += r1[d][i, t, :, near_cut].astype(jnp.float32)
            if k == 0:
                total += other[d][i, t, :, raw_cut].astype(jnp.float32)
        return total

    def by_block(scalars):
        return jnp.concatenate([jnp.full((block_rows, LANES), s) for s in scalars], axis=0)

    for s in states:
        s.wait()
    layers = [layer_ref[0, b] for b in range(blocks)]
    lives = [valid_ref[0, b] for b in range(blocks)]
    row_decay = by_block([decay_ref[layer] for layer in layers])
    row_live = by_block([jnp.where(v > 0, 1.0, 0.0).astype(jnp.float32) for v in lives]) > 0.5
    n_layer = decay_ref.shape[0]
    lane = lax.broadcasted_iota(jnp.int32, (1, LANES), 1)

    def by_layer(values, offset):
        terms = []
        for b in range(blocks):
            chosen = jnp.where(lives[b] > 0, layers[b] + offset, -1)
            block = values[b * block_rows : (b + 1) * block_rows]
            terms.append(jnp.where(lane == chosen, jnp.sum(block, axis=1, keepdims=True), 0.0))
        return jnp.sum(sum(terms[1:], terms[0]), axis=0, keepdims=True)

    def weigh(i, wsum):
        weights = p_v[:, pl.ds(pl.multiple_of(i * LANES, LANES), LANES)].astype(jnp.float32)
        return wsum + weights * weights

    zero = jnp.zeros((rows, LANES), jnp.float32)
    weight_line = by_layer(lax.fori_loop(0, cols // LANES, weigh, zero, unroll=2), 0)

    twos = {}
    for k in range(count):
        for d in range(2):
            with jax.named_scope(f"onew{k}{d}"):
                for c in ones[k, d]:
                    c.wait_recv()
                if k == 0:

                    @pl.when(is_near)
                    def _(d=d):
                        for c in raws[d]:
                            c.wait_recv()

            group = []
            for j in range(1, second_n[d]):
                at_hand = y if d == 0 else x
                t = lax.rem(at_hand + j, second_n[d])
                total = partial(k, d, t, span(k, d), inner(k), slice(None))
                s1[d][j - 1, :, inner(k)] = total.astype(jnp.bfloat16)
                c = pltpu.make_async_remote_copy(
                    src_ref=s1[d].at[j - 1, :, inner(k)], dst_ref=r2[d].at[j - 1, :, inner(k)],
                    send_sem=two_send.at[k, d, j - 1], recv_sem=two_recv.at[k, d, j - 1],
                    device_id=peer_at(1 - d, t, core), device_id_type=MESH,
                )
                c.start()
                group.append(c)
            twos[k, d] = group
        if 0 < k <= n_sec:
            relay(k)
    for k in range(count, n_sec + 1):
        relay(k)

    for d in range(2):
        for k in range(count):
            if k not in (0, SHIFT):
                pair[k, d].wait_send()

        @pl.when(is_near)
        def _(d=d):
            for c in (pair[0, d], kept[SHIFT, d], *ones[SHIFT, d], *crosses[d]):
                c.wait_send()

        @pl.when(is_far)
        def _(d=d):
            for c in (kept[0, d], pair[SHIFT, d], *lends[d], *raws[d]):
                c.wait_send()

    def lanes(start):
        return pl.ds(start if isinstance(start, int) else pl.multiple_of(start, LANES), LANES)

    usum = zero
    for k in range(count):
        for d in range(2):
            with jax.named_scope(f"twow{k}{d}"):
                for c in twos[k, d]:
                    c.wait_recv()

            def update_piece(i, usum, k=k, d=d):
                raw_cut, near_cut, cut = (lanes(base + i * LANES) for base in (0, starts[k], d * half + starts[k]))
                grad = partial(k, d, y if d == 0 else x, cut, near_cut, raw_cut)
                for j in range(second_n[d] - 1):
                    grad += r2[d][j, :, near_cut].astype(jnp.float32)
                weights = p_v[:, cut].astype(jnp.float32)
                old1, old2 = m1_v[:, cut], m2_v[:, cut]
                tenth = 0.1 * grad
                first = 0.9 * old1 + tenth
                second = 0.99 * old2 + tenth * tenth
                root = second * lax.rsqrt(second)
                update = first * (root_second / bias_first) / (root + 1e-06 * root_second) + row_decay * weights
                upd[:, cut] = update
                new1_ref[:, cut] = jnp.where(row_live, first, old1)
                new2_ref[:, cut] = jnp.where(row_live, second, old2)
                return usum + update * update

            n = (cuts[k] - starts[k]) // LANES

            def update_block(i, usum):
                for u in range(WIDE):
                    usum = update_piece(i * WIDE + u, usum)
                return usum

            with jax.named_scope(f"upd{k}{d}"):
                usum = lax.fori_loop(0, n // WIDE, update_block, usum)
                for i in range(n // WIDE * WIDE, n):
                    usum = update_piece(i, usum)

    line = weight_line + by_layer(usum, n_layer)

    def all_sum(line, slots, send_sem, recv_sem, index, peers, sent):
        slots[index] = line
        for peer in peers:
            pltpu.make_async_remote_copy(
                src_ref=slots.at[index], dst_ref=slots.at[index],
                send_sem=send_sem.at[0], recv_sem=recv_sem.at[0],
                device_id=peer, device_id_type=MESH,
            ).start()
        whole = slots.at[pl.ds(0, len(peers))]
        both = pltpu.make_async_remote_copy(
            src_ref=whole, dst_ref=whole, send_sem=send_sem.at[0], recv_sem=recv_sem.at[0],
            device_id=peers[0], device_id_type=MESH,
        )
        if sent:
            with jax.named_scope("endw"):
                for c in sent:
                    c.wait_send()
        with jax.named_scope("allw"):
            both.wait_recv()
        terms = [slots[j] for j in range(len(peers) + 1)]
        while len(terms) > 1:
            terms = [sum(terms[i + 1 : i + 2], terms[i]) for i in range(0, len(terms), 2)]
        return terms[0], both

    groups = (*(ones[k, d] for k in range(count) if k != SHIFT for d in range(2)), *twos.values())
    sent = [c for group in groups for c in group]
    if one_shot:
        every = [
            (i + jnp.where(i >= sec, 1, 0), j) for i in range(n_sec - 1) for j in range(n_shard)
        ] + [(sec, lax.rem(me + j, n_shard)) for j in range(1, n_shard)]
        line, last = all_sum(line, tiles, t_send, t_recv, sec * n_shard + me, every, sent)
        sends = [last]
    else:
        shard_peers = [(sec, lax.rem(me + j, n_shard)) for j in range(1, n_shard)]
        sec_peers = [(lax.rem(sec + j, n_sec), me) for j in range(1, n_sec)]
        line, last = all_sum(line, tiles, t_send, t_recv, me, shard_peers, sent)
        line, zlast = all_sum(line, ztiles, z_send, z_recv, sec, sec_peers, [])
        sends = [last, zlast]
    ratios = jnp.sqrt(line / (pltpu.roll(line, LANES - n_layer, 1) + 1.0))
    ratio_ref[...] = ratios[0, :n_layer]
    step_ref[...] = jnp.concatenate(
        [
            jnp.broadcast_to(
                0.1 * jnp.sum(
                    jnp.where((lane == layers[b]) & (lives[b] > 0), ratios, 0.0), axis=1, keepdims=True
                ),
                (block_rows, LANES),
            )
            for b in range(blocks)
        ],
        axis=0,
    )
    for c in sends:
        c.wait_send()


def finish(parts, p_v, upd, new1_v, new2_v, step_v, ratio_v, newp_hbm, new1_hbm, new2_hbm, ratio_hbm, newp_v, sem):
    cols = p_v.shape[1]
    width = cols // parts
    copies = [pltpu.make_async_copy(ratio_v, ratio_hbm, sem.at[0])]
    for k in range(parts):
        span = pl.ds(k * width, width)
        for i, (src, dst) in enumerate(((new1_v, new1_hbm), (new2_v, new2_hbm))):
            copies.append(pltpu.make_async_copy(src.at[:, span], dst.at[:, span], sem.at[1 + i * parts + k]))
    for c in copies:
        c.start()
    row_step = step_v[...]

    for k in range(parts):
        def step_piece(i, carry, k=k):
            outer = pl.ds(pl.multiple_of(k * width + i * LANES, LANES), LANES)
            stepped = p_v[:, outer].astype(jnp.float32) - row_step * upd[:, outer]
            newp_v[:, outer] = stepped.astype(jnp.bfloat16)
            return carry

        lax.fori_loop(0, width // LANES, step_piece, 0, unroll=4)
        span = pl.ds(k * width, width)
        c = pltpu.make_async_copy(newp_v.at[:, span], newp_hbm.at[:, span], sem.at[1 + 2 * parts + k])
        c.start()
        copies.append(c)
    for c in copies:
        c.wait()


def shards(grad_parts, params, moment_first, moment_second, block_layer, block_valid, decay):
    n_sec, n_shard = lax.axis_size("section"), lax.axis_size("shard")
    chips = n_shard // 2
    n_y = max(d for d in range(1, math.isqrt(chips) + 1) if chips % d == 0)
    n_x = chips // n_y
    rows, cols = params.shape[1:]
    n_layer = decay.shape[0]
    half = cols // 2
    cuts = tuple(half // LANES * c // CUTS[-1] * LANES for c in CUTS)
    bf16, f32 = jnp.bfloat16, jnp.float32
    dma = pltpu.SemaphoreType.DMA
    one_shot = ONE_SHOT and n_shard * n_sec <= 32
    n_lines = n_shard * n_sec if one_shot else n_shard
    grads = grad_parts.reshape(n_y, n_x, 2, rows, cols)
    any_spec = pl.BlockSpec(memory_space=pltpu.HBM)
    vmem = pl.BlockSpec(memory_space=pltpu.VMEM)
    held = pl.pallas_call(
        functools.partial(kernel, n_sec, n_y, n_x, cuts),
        out_shape=(
            pltpu.VMEM((rows, cols), bf16),
            pltpu.VMEM((rows, cols), f32),
            pltpu.VMEM((rows, cols), f32),
            pltpu.VMEM((rows, cols), f32),
            pltpu.VMEM((rows, LANES), f32),
            pltpu.VMEM((n_layer,), f32),
        ),
        in_specs=[any_spec] * 7,
        out_specs=(vmem,) * 6,
        scratch_shapes=[
            pltpu.VMEM((n_y, n_x, 2, rows, cols), bf16),
            pltpu.VMEM((n_y, n_x, rows, cols), bf16),
            pltpu.VMEM((rows, cols), f32),
            pltpu.VMEM((rows, cols), f32),
            pltpu.VMEM((n_x - 1, n_y, rows, half), bf16),
            pltpu.VMEM((n_y - 1, n_x, rows, half), bf16),
            pltpu.VMEM((n_y - 1, rows, half), bf16),
            pltpu.VMEM((n_x - 1, rows, half), bf16),
            pltpu.VMEM((n_y - 1, rows, half), bf16),
            pltpu.VMEM((n_x - 1, rows, half), bf16),
            pltpu.VMEM((n_x - 1, n_y, rows, cuts[0]), bf16),
            pltpu.VMEM((n_y - 1, n_x, rows, cuts[0]), bf16),
            pltpu.VMEM((n_x - 1, n_y, rows, cuts[SHIFT] - cuts[SHIFT - 1]), bf16),
            pltpu.VMEM((n_y - 1, n_x, rows, cuts[SHIFT] - cuts[SHIFT - 1]), bf16),
            pltpu.VMEM((n_lines, 1, LANES), f32),
            None if one_shot else pltpu.VMEM((n_sec, 1, LANES), f32),
            pltpu.SMEM(block_layer.shape, jnp.int32),
            pltpu.SMEM(block_valid.shape, jnp.int32),
            pltpu.SMEM(decay.shape, f32),
        ],
        compiler_params=pltpu.CompilerParams(
            collective_id=0, has_side_effects=True, vmem_limit_bytes=56 * 1024 * 1024
        ),
    )(grads, params[0], moment_first[0], moment_second[0], block_layer, block_valid, decay)
    out = pl.pallas_call(
        functools.partial(finish, PARTS),
        out_shape=(
            jax.ShapeDtypeStruct((rows, cols), bf16),
            jax.ShapeDtypeStruct((rows, cols), f32),
            jax.ShapeDtypeStruct((rows, cols), f32),
            jax.ShapeDtypeStruct((n_layer,), f32),
        ),
        in_specs=[vmem] * 6,
        out_specs=(any_spec,) * 4,
        scratch_shapes=[pltpu.VMEM((rows, cols), bf16), dma((1 + 3 * PARTS,))],
        compiler_params=pltpu.CompilerParams(vmem_limit_bytes=8 * 1024 * 1024),
    )(*held)
    return (out[0][None], out[1][None], out[2][None], out[3])


def solution(mesh):
    placed = (
        P("section", "shard", None, None),
        P("section", "shard", None),
        P("section", "shard", None),
        P("section", "shard", None),
        P("section", "shard"),
        P("section", "shard"),
        P(),
    )
    return jax.shard_map(
        shards,
        mesh=mesh,
        in_specs=placed,
        out_specs=(
            P("section", "shard", None),
            P("section", "shard", None),
            P("section", "shard", None),
            P(),
        ),
        check_vma=False,
    )
```

```python
import functools
import math

import jax
import jax.numpy as jnp
from jax import lax
from jax.experimental import pallas as pl
from jax.experimental.pallas import tpu as pltpu
from jax.sharding import PartitionSpec as P

MESH = pl.DeviceIdType.MESH
bias_first = 1.0 - 0.9**10
bias_second = 1.0 - 0.99**10
root_second = math.sqrt(bias_second)
LANES = 128
CUTS = (3, 5, 9, 17, 24, 28, 31, 32)
SHIFT = 2
ONE_SHOT = True
PARTS = 2
WIDE = 4


def kernel(
    n_sec, n_y, n_x, cuts,
    g_hbm, p_hbm, m1_hbm, m2_hbm, layer_hbm, valid_hbm, decay_hbm,
    p_v, upd, new1_ref, new2_ref, chosen_ref, total_ref,
    mine, d2d, m1_v, m2_v, r1x, r1y, s1x, s1y, r2x, r2y, xa, ya, xs, ys, tiles, ztiles, layer_ref, valid_ref, decay_ref,
):
    count = len(cuts)
    most = max(n_x, n_y) - 1
    one_shot = ztiles is None
    dma = pltpu.SemaphoreType.DMA
    pl.run_scoped(
        functools.partial(
            body, n_sec, n_y, n_x, cuts, one_shot,
            g_hbm, p_hbm, m1_hbm, m2_hbm, layer_hbm, valid_hbm, decay_hbm,
            p_v, upd, new1_ref, new2_ref, chosen_ref, total_ref,
            mine, d2d, m1_v, m2_v, (r1x, r1y), (s1x, s1y), (r2x, r2y), (xa, ya), (xs, ys), tiles, ztiles,
            layer_ref, valid_ref, decay_ref,
        ),
        load_sem=dma((count, 2)),
        state_sem=dma((6,)),
        pair_send=dma((count, 2)),
        one_send=dma((count, 2, most)),
        two_send=dma((count, 2, most)),
        raw_send=dma((2, most)),
        lent_send=dma((2, 2, most)),
        lent_recv=dma((2, most)),
        t_send=dma((1,)),
        z_send=dma((1,)),
        pair_recv=dma((count, 2)),
        one_recv=dma((count, 2, most)),
        two_recv=dma((count, 2, most)),
        raw_recv=dma((2, most)),
        t_recv=dma((1,)),
        z_recv=dma((1,)),
        told=pltpu.SemaphoreType.REGULAR((2, n_sec - 1)),
        inside=pltpu.SemaphoreType.REGULAR,
        whole=pltpu.SemaphoreType.REGULAR,
        settled=pltpu.SemaphoreType.REGULAR,
    )


def body(
    n_sec, n_y, n_x, cuts, one_shot,
    g_hbm, p_hbm, m1_hbm, m2_hbm, layer_hbm, valid_hbm, decay_hbm,
    p_v, upd, new1_ref, new2_ref, chosen_ref, total_ref,
    mine, d2d, m1_v, m2_v, r1, s1, r2, other, lent, tiles, ztiles, layer_ref, valid_ref, decay_ref,
    load_sem, state_sem, pair_send, one_send, two_send, raw_send, lent_send, lent_recv, t_send, z_send,
    pair_recv, one_recv, two_recv, raw_recv, t_recv, z_recv, told, inside, whole, settled,
):
    rows, cols = p_v.shape
    half = cols // 2
    count = len(cuts)
    n_shard = 2 * n_y * n_x
    sec, me = lax.axis_index("section"), lax.axis_index("shard")
    core = lax.rem(me, 2)
    is_far, is_near = core == 0, core == 1
    x = lax.rem(me // 2, n_x)
    y = me // (2 * n_x)
    blocks = layer_ref.shape[1]
    block_rows = rows // blocks

    def at(yy, xx, cc):
        return (sec, (yy * n_x + xx) * 2 + cc)

    starts = (0,) + cuts[:-1]

    def span(k, d):
        return pl.ds(d * half + starts[k], cuts[k] - starts[k])

    def inner(k):
        return pl.ds(starts[k], cuts[k] - starts[k])

    order = [1, 0, *range(2, count)]
    loads = {}
    for k in order:
        for d in range(2):
            c = pltpu.make_async_copy(
                g_hbm.at[:, :, :, :, span(k, d)], mine.at[:, :, :, :, span(k, d)], load_sem.at[k, d]
            )
            c.start()
            loads[k, d] = c
        if k == 1:
            barrier = pltpu.get_barrier_semaphore()
            beside = at(y, x, 1 - core)
            around = [at(y, lax.rem(x + j, n_x), core) for j in range(1, n_x)]
            around += [at(lax.rem(y + j, n_y), x, core) for j in range(1, n_y)]
            last_sec = n_sec - 1
            up = (jnp.minimum(sec + 1, last_sec), me)
            down = (jnp.maximum(sec - 1, 0), me)
            ends = jnp.where(sec < last_sec, 1, 0) + jnp.where(sec > 0, 1, 0)

            def tell(semaphore):
                for peer in around:
                    pl.semaphore_signal(semaphore, inc=1, device_id=peer, device_id_type=MESH)

                @pl.when(sec < last_sec)
                def _():
                    pl.semaphore_signal(semaphore, inc=1, device_id=up, device_id_type=MESH)

                @pl.when(sec > 0)
                def _():
                    pl.semaphore_signal(semaphore, inc=1, device_id=down, device_id_type=MESH)

            @pl.when(is_near)
            def _():
                tell(barrier)
                pl.semaphore_signal(barrier, inc=1, device_id=beside, device_id_type=MESH)

    states = [
        pltpu.make_async_copy(src, dst, state_sem.at[i])
        for i, (src, dst) in enumerate(
            (
                (layer_hbm, layer_ref), (valid_hbm, valid_ref), (decay_hbm, decay_ref),
                (p_hbm, p_v), (m1_hbm, m1_v), (m2_hbm, m2_v),
            )
        )
    ]
    for s in states:
        s.start()

    @pl.when(is_far)
    def _():
        pl.semaphore_wait(barrier, 1)
        pl.semaphore_signal(inside, inc=1, device_id=beside, device_id_type=MESH)
        for d in range(2):
            other[d][...] = jnp.zeros_like(other[d])

    @pl.when(is_near)
    def _():
        with jax.named_scope("bar1"):
            pl.semaphore_wait(inside, 1)
            pl.semaphore_wait(barrier, len(around) + ends)
        tell(whole)
        pl.semaphore_signal(inside, inc=1, device_id=beside, device_id_type=MESH)

    def meet():
        with jax.named_scope("bar"):

            @pl.when(is_near)
            def _():
                pl.semaphore_wait(whole, len(around) + ends)
                pl.semaphore_signal(settled, inc=1, device_id=beside, device_id_type=MESH)

            @pl.when(is_far)
            def _():
                pl.semaphore_wait(settled, 1)

    def relay(d):
        if 1 < d <= n_sec:

            @pl.when(sec >= d - 1)
            def _():
                pl.semaphore_wait(told.at[0, d - 2], 1)

            @pl.when(sec <= n_sec - d)
            def _():
                pl.semaphore_wait(told.at[1, d - 2], 1)

        if d < n_sec:

            @pl.when((sec >= d - 1) & (sec < last_sec))
            def _():
                pl.semaphore_signal(told.at[0, d - 1], inc=1, device_id=up, device_id_type=MESH)

            @pl.when((sec <= n_sec - d) & (sec > 0))
            def _():
                pl.semaphore_signal(told.at[1, d - 1], inc=1, device_id=down, device_id_type=MESH)

    def place(d, t):
        return (slice(None), t) if d == 0 else (t, slice(None))

    def peer_at(d, t, cc):
        return at(y, t, cc) if d == 0 else at(t, x, cc)

    here = (x, y)
    first_n, second_n = (n_x, n_y), (n_y, n_x)

    def others(d):
        return [(j, lax.rem(here[d] + j, first_n[d])) for j in range(1, first_n[d])]

    def remote(src, dst, send_sem, recv_sem, peer):
        return pltpu.make_async_remote_copy(
            src_ref=src, dst_ref=dst, send_sem=send_sem, recv_sem=recv_sem, device_id=peer, device_id_type=MESH
        )

    def rows_of(d, t, cc, k):
        return mine.at[(*place(d, t), cc, slice(None), span(k, d))]

    ones, raws, lends, crosses, pair, kept = {}, {}, {}, {}, {}, {}
    for d in range(2):
        for k in range(count):
            ones[k, d] = [
                remote(
                    rows_of(d, t, core, k), r1[d].at[j - 1, :, :, inner(k)],
                    one_send.at[k, d, j - 1], one_recv.at[k, d, j - 1], peer_at(d, t, core),
                )
                for j, t in others(d)
            ]
            for group, t in ((pair, slice(None)), (kept, here[d])):
                if group is kept and k not in (0, SHIFT):
                    continue
                spot = place(d, t)
                group[k, d] = remote(
                    rows_of(d, t, 1 - core, k), d2d.at[(*spot, slice(None), span(k, d))],
                    pair_send.at[k, d], pair_recv.at[k, d], at(y, x, 1 - core),
                )
        raws[d] = [
            remote(
                rows_of(d, t, 1 - core, 0), other[d].at[j - 1],
                raw_send.at[d, j - 1], raw_recv.at[d, j - 1], peer_at(d, t, 1 - core),
            )
            for j, t in others(d)
        ]
        lends[d] = [
            remote(
                rows_of(d, t, core, SHIFT), lent[d].at[j - 1],
                lent_send.at[0, d, j - 1], lent_recv.at[d, j - 1], at(y, x, 1 - core),
            )
            for j, t in others(d)
        ]
        crosses[d] = [
            remote(
                rows_of(d, t, 1 - core, SHIFT), r1[d].at[j - 1, :, :, inner(SHIFT)],
                lent_send.at[1, d, j - 1], one_recv.at[SHIFT, d, j - 1], peer_at(d, t, 1 - core),
            )
            for j, t in others(d)
        ]

    def send_pair(k, d):
        if k:
            with jax.named_scope(f"ldw{k}{d}"):
                loads[k, d].wait()
        if k == 0:

            @pl.when(is_far)
            def _():
                loads[k, d].wait()
                kept[k, d].start()

            @pl.when(is_near)
            def _():
                pair[k, d].start()
        elif k == SHIFT:

            @pl.when(is_far)
            def _():
                for c in (pair[k, d], *lends[d]):
                    c.start()

            @pl.when(is_near)
            def _():
                kept[k, d].start()
        else:
            pair[k, d].start()

    def add_pair(yy, xx, cut):
        total = mine[yy, xx, core, :, cut].astype(jnp.float32) + d2d[yy, xx, :, cut].astype(jnp.float32)
        mine[yy, xx, core, :, cut] = total.astype(jnp.bfloat16)

    def add_all(cut):
        def add_one(i, carry):
            add_pair(i // n_x, lax.rem(i, n_x), cut)
            return carry

        lax.fori_loop(0, n_y * n_x, add_one, 0)

    def add_kept(d, cut):
        for i in range(second_n[d]):
            add_pair(i if d == 0 else y, x if d == 0 else i, cut)

    def send_one(k, d):
        cut = span(k, d)
        if k == 0:

            @pl.when(is_near)
            def _():
                kept[k, d].wait_recv()
                add_kept(d, cut)

            @pl.when(is_far)
            def _():
                pair[k, d].wait_recv()
                add_all(cut)
                for c in ones[k, d]:
                    c.start()

        elif k == SHIFT:

            @pl.when(is_near)
            def _():
                pair[k, d].wait_recv()
                for c in lends[d]:
                    c.wait_recv()
                add_all(cut)
                for c in ones[k, d]:
                    c.start()
                for j, t in others(d):
                    for i in range(second_n[d]):
                        yy, xx = (i, t) if d == 0 else (t, i)
                        total = mine[yy, xx, 1 - core, :, cut].astype(jnp.float32)
                        total += lent[d][j - 1, i].astype(jnp.float32)
                        mine[yy, xx, 1 - core, :, cut] = total.astype(jnp.bfloat16)
                for c in crosses[d]:
                    c.start()

            @pl.when(is_far)
            def _():
                kept[k, d].wait_recv()
                add_kept(d, cut)
        else:
            with jax.named_scope(f"pairw{k}{d}"):
                pair[k, d].wait_recv()
            add_all(cut)
            for c in ones[k, d]:
                c.start()

    @pl.when(is_near)
    def _():
        for d in range(2):
            loads[0, d].wait()
            for c in ones[0, d]:
                c.start()

    ahead = 3
    for i, k in enumerate(order[: 1 + ahead]):
        if i == 2:

            @pl.when(is_far)
            def _():
                pl.semaphore_wait(inside, 1)
                for d in range(2):
                    for c in raws[d]:
                        c.start()

            meet()
        for d in range(2):
            send_pair(k, d)
    for i, k in enumerate(order):
        for d in range(2):
            send_one(k, d)
        if i + 1 + ahead < count:
            for d in range(2):
                send_pair(order[i + 1 + ahead], d)

    def partial(k, d, t, cut, near_cut, raw_cut):
        yy, xx = (t, x) if d == 0 else (y, t)
        total = mine[yy, xx, core, :, cut].astype(jnp.float32)
        for i in range(first_n[d] - 1):
            total += r1[d][i, t, :, near_cut].astype(jnp.float32)
            if k == 0:
                total += other[d][i, t, :, raw_cut].astype(jnp.float32)
        return total

    def by_block(scalars):
        return jnp.concatenate([jnp.full((block_rows, LANES), s) for s in scalars], axis=0)

    for s in states:
        s.wait()
    layers = [layer_ref[0, b] for b in range(blocks)]
    lives = [valid_ref[0, b] for b in range(blocks)]
    row_decay = by_block([decay_ref[layer] for layer in layers])
    row_live = by_block([jnp.where(v > 0, 1.0, 0.0).astype(jnp.float32) for v in lives]) > 0.5
    n_layer = decay_ref.shape[0]
    lane = lax.broadcasted_iota(jnp.int32, (1, LANES), 1)

    def by_layer(values, offset):
        terms = []
        for b in range(blocks):
            chosen = jnp.where(lives[b] > 0, layers[b] + offset, -1)
            block = values[b * block_rows : (b + 1) * block_rows]
            terms.append(jnp.where(lane == chosen, jnp.sum(block, axis=1, keepdims=True), 0.0))
        return jnp.sum(sum(terms[1:], terms[0]), axis=0, keepdims=True)

    def weigh(i, wsum):
        weights = p_v[:, pl.ds(pl.multiple_of(i * LANES, LANES), LANES)].astype(jnp.float32)
        return wsum + weights * weights

    zero = jnp.zeros((rows, LANES), jnp.float32)
    chosen_ref[...] = jnp.concatenate(
        [
            jnp.broadcast_to(jnp.where((lane == layers[b]) & (lives[b] > 0), 0.1, 0.0), (block_rows, LANES))
            for b in range(blocks)
        ],
        axis=0,
    )
    weight_line = by_layer(lax.fori_loop(0, cols // LANES, weigh, zero, unroll=2), 0)

    twos = {}
    for k in range(count):
        for d in range(2):
            with jax.named_scope(f"onew{k}{d}"):
                for c in ones[k, d]:
                    c.wait_recv()
                if k == 0:

                    @pl.when(is_near)
                    def _(d=d):
                        for c in raws[d]:
                            c.wait_recv()

            group = []
            for j in range(1, second_n[d]):
                at_hand = y if d == 0 else x
                t = lax.rem(at_hand + j, second_n[d])
                total = partial(k, d, t, span(k, d), inner(k), slice(None))
                s1[d][j - 1, :, inner(k)] = total.astype(jnp.bfloat16)
                c = pltpu.make_async_remote_copy(
                    src_ref=s1[d].at[j - 1, :, inner(k)], dst_ref=r2[d].at[j - 1, :, inner(k)],
                    send_sem=two_send.at[k, d, j - 1], recv_sem=two_recv.at[k, d, j - 1],
                    device_id=peer_at(1 - d, t, core), device_id_type=MESH,
                )
                c.start()
                group.append(c)
            twos[k, d] = group
        if 0 < k <= n_sec:
            relay(k)
    for k in range(count, n_sec + 1):
        relay(k)

    for d in range(2):
        for k in range(count):
            if k not in (0, SHIFT):
                pair[k, d].wait_send()

        @pl.when(is_near)
        def _(d=d):
            for c in (pair[0, d], kept[SHIFT, d], *ones[SHIFT, d], *crosses[d]):
                c.wait_send()

        @pl.when(is_far)
        def _(d=d):
            for c in (kept[0, d], pair[SHIFT, d], *lends[d], *raws[d]):
                c.wait_send()

    def lanes(start):
        return pl.ds(start if isinstance(start, int) else pl.multiple_of(start, LANES), LANES)

    usum = zero
    for k in range(count):
        for d in range(2):
            with jax.named_scope(f"twow{k}{d}"):
                for c in twos[k, d]:
                    c.wait_recv()

            def update_piece(i, usum, k=k, d=d):
                raw_cut, near_cut, cut = (lanes(base + i * LANES) for base in (0, starts[k], d * half + starts[k]))
                grad = partial(k, d, y if d == 0 else x, cut, near_cut, raw_cut)
                for j in range(second_n[d] - 1):
                    grad += r2[d][j, :, near_cut].astype(jnp.float32)
                weights = p_v[:, cut].astype(jnp.float32)
                old1, old2 = m1_v[:, cut], m2_v[:, cut]
                tenth = 0.1 * grad
                first = 0.9 * old1 + tenth
                second = 0.99 * old2 + tenth * tenth
                root = second * lax.rsqrt(second)
                update = first * (root_second / bias_first) / (root + 1e-06 * root_second) + row_decay * weights
                upd[:, cut] = update
                new1_ref[:, cut] = jnp.where(row_live, first, old1)
                new2_ref[:, cut] = jnp.where(row_live, second, old2)
                return usum + update * update

            n = (cuts[k] - starts[k]) // LANES

            def update_block(i, usum):
                for u in range(WIDE):
                    usum = update_piece(i * WIDE + u, usum)
                return usum

            with jax.named_scope(f"upd{k}{d}"):
                usum = lax.fori_loop(0, n // WIDE, update_block, usum)
                for i in range(n // WIDE * WIDE, n):
                    usum = update_piece(i, usum)

    line = weight_line + by_layer(usum, n_layer)

    def all_sum(line, slots, send_sem, recv_sem, index, peers, sent):
        slots[index] = line
        for peer in peers:
            pltpu.make_async_remote_copy(
                src_ref=slots.at[index], dst_ref=slots.at[index],
                send_sem=send_sem.at[0], recv_sem=recv_sem.at[0],
                device_id=peer, device_id_type=MESH,
            ).start()
        whole = slots.at[pl.ds(0, len(peers))]
        both = pltpu.make_async_remote_copy(
            src_ref=whole, dst_ref=whole, send_sem=send_sem.at[0], recv_sem=recv_sem.at[0],
            device_id=peers[0], device_id_type=MESH,
        )
        if sent:
            with jax.named_scope("endw"):
                for c in sent:
                    c.wait_send()
        with jax.named_scope("allw"):
            both.wait_recv()
        terms = [slots[j] for j in range(len(peers) + 1)]
        while len(terms) > 1:
            terms = [sum(terms[i + 1 : i + 2], terms[i]) for i in range(0, len(terms), 2)]
        return terms[0], both

    groups = (*(ones[k, d] for k in range(count) if k != SHIFT for d in range(2)), *twos.values())
    sent = [c for group in groups for c in group]
    if one_shot:
        every = [
            (i + jnp.where(i >= sec, 1, 0), j) for i in range(n_sec - 1) for j in range(n_shard)
        ] + [(sec, lax.rem(me + j, n_shard)) for j in range(1, n_shard)]
        line, last = all_sum(line, tiles, t_send, t_recv, sec * n_shard + me, every, sent)
        sends = [last]
    else:
        shard_peers = [(sec, lax.rem(me + j, n_shard)) for j in range(1, n_shard)]
        sec_peers = [(lax.rem(sec + j, n_sec), me) for j in range(1, n_sec)]
        line, last = all_sum(line, tiles, t_send, t_recv, me, shard_peers, sent)
        line, zlast = all_sum(line, ztiles, z_send, z_recv, sec, sec_peers, [])
        sends = [last, zlast]
    total_ref[...] = line
    for c in sends:
        c.wait_send()


def finish(
    parts, p_v, upd, new1_v, new2_v, chosen_v, total_v, newp_hbm, new1_hbm, new2_hbm, ratio_hbm, newp_v, ratio_v, sem
):
    cols = p_v.shape[1]
    width = cols // parts
    copies = []
    for k in range(parts):
        span = pl.ds(k * width, width)
        for i, (src, dst) in enumerate(((new1_v, new1_hbm), (new2_v, new2_hbm))):
            copies.append(pltpu.make_async_copy(src.at[:, span], dst.at[:, span], sem.at[1 + i * parts + k]))
    for c in copies:
        c.start()
    total = total_v[...]
    n_layer = ratio_v.shape[0]
    ratios = jnp.sqrt(total / (pltpu.roll(total, LANES - n_layer, 1) + 1.0))
    ratios = jnp.where(lax.broadcasted_iota(jnp.int32, ratios.shape, 1) < n_layer, ratios, 0.0)
    row_step = jnp.broadcast_to(jnp.sum(chosen_v[...] * ratios, axis=1, keepdims=True), chosen_v.shape)
    ratio_v[...] = ratios[0, :n_layer]
    copies.append(pltpu.make_async_copy(ratio_v, ratio_hbm, sem.at[0]))
    copies[-1].start()

    for k in range(parts):
        def step_piece(i, carry, k=k):
            outer = pl.ds(pl.multiple_of(k * width + i * LANES, LANES), LANES)
            stepped = p_v[:, outer].astype(jnp.float32) - row_step * upd[:, outer]
            newp_v[:, outer] = stepped.astype(jnp.bfloat16)
            return carry

        lax.fori_loop(0, width // LANES, step_piece, 0, unroll=4)
        span = pl.ds(k * width, width)
        c = pltpu.make_async_copy(newp_v.at[:, span], newp_hbm.at[:, span], sem.at[1 + 2 * parts + k])
        c.start()
        copies.append(c)
    for c in copies:
        c.wait()


def shards(grad_parts, params, moment_first, moment_second, block_layer, block_valid, decay):
    n_sec, n_shard = lax.axis_size("section"), lax.axis_size("shard")
    chips = n_shard // 2
    n_y = max(d for d in range(1, math.isqrt(chips) + 1) if chips % d == 0)
    n_x = chips // n_y
    rows, cols = params.shape[1:]
    n_layer = decay.shape[0]
    half = cols // 2
    cuts = tuple(half // LANES * c // CUTS[-1] * LANES for c in CUTS)
    bf16, f32 = jnp.bfloat16, jnp.float32
    dma = pltpu.SemaphoreType.DMA
    one_shot = ONE_SHOT and n_shard * n_sec <= 32
    n_lines = n_shard * n_sec if one_shot else n_shard
    grads = grad_parts.reshape(n_y, n_x, 2, rows, cols)
    any_spec = pl.BlockSpec(memory_space=pltpu.HBM)
    vmem = pl.BlockSpec(memory_space=pltpu.VMEM)
    held = pl.pallas_call(
        functools.partial(kernel, n_sec, n_y, n_x, cuts),
        out_shape=(
            pltpu.VMEM((rows, cols), bf16),
            pltpu.VMEM((rows, cols), f32),
            pltpu.VMEM((rows, cols), f32),
            pltpu.VMEM((rows, cols), f32),
            pltpu.VMEM((rows, LANES), f32),
            pltpu.VMEM((1, LANES), f32),
        ),
        in_specs=[any_spec] * 7,
        out_specs=(vmem,) * 6,
        scratch_shapes=[
            pltpu.VMEM((n_y, n_x, 2, rows, cols), bf16),
            pltpu.VMEM((n_y, n_x, rows, cols), bf16),
            pltpu.VMEM((rows, cols), f32),
            pltpu.VMEM((rows, cols), f32),
            pltpu.VMEM((n_x - 1, n_y, rows, half), bf16),
            pltpu.VMEM((n_y - 1, n_x, rows, half), bf16),
            pltpu.VMEM((n_y - 1, rows, half), bf16),
            pltpu.VMEM((n_x - 1, rows, half), bf16),
            pltpu.VMEM((n_y - 1, rows, half), bf16),
            pltpu.VMEM((n_x - 1, rows, half), bf16),
            pltpu.VMEM((n_x - 1, n_y, rows, cuts[0]), bf16),
            pltpu.VMEM((n_y - 1, n_x, rows, cuts[0]), bf16),
            pltpu.VMEM((n_x - 1, n_y, rows, cuts[SHIFT] - cuts[SHIFT - 1]), bf16),
            pltpu.VMEM((n_y - 1, n_x, rows, cuts[SHIFT] - cuts[SHIFT - 1]), bf16),
            pltpu.VMEM((n_lines, 1, LANES), f32),
            None if one_shot else pltpu.VMEM((n_sec, 1, LANES), f32),
            pltpu.SMEM(block_layer.shape, jnp.int32),
            pltpu.SMEM(block_valid.shape, jnp.int32),
            pltpu.SMEM(decay.shape, f32),
        ],
        compiler_params=pltpu.CompilerParams(
            collective_id=0, has_side_effects=True, vmem_limit_bytes=56 * 1024 * 1024
        ),
    )(grads, params[0], moment_first[0], moment_second[0], block_layer, block_valid, decay)
    out = pl.pallas_call(
        functools.partial(finish, PARTS),
        out_shape=(
            jax.ShapeDtypeStruct((rows, cols), bf16),
            jax.ShapeDtypeStruct((rows, cols), f32),
            jax.ShapeDtypeStruct((rows, cols), f32),
            jax.ShapeDtypeStruct((n_layer,), f32),
        ),
        in_specs=[vmem] * 6,
        out_specs=(any_spec,) * 4,
        scratch_shapes=[pltpu.VMEM((rows, cols), bf16), pltpu.VMEM((n_layer,), f32), dma((1 + 3 * PARTS,))],
        compiler_params=pltpu.CompilerParams(vmem_limit_bytes=8 * 1024 * 1024),
    )(*held)
    return (out[0][None], out[1][None], out[2][None], out[3])


def solution(mesh):
    placed = (
        P("section", "shard", None, None),
        P("section", "shard", None),
        P("section", "shard", None),
        P("section", "shard", None),
        P("section", "shard"),
        P("section", "shard"),
        P(),
    )
    return jax.shard_map(
        shards,
        mesh=mesh,
        in_specs=placed,
        out_specs=(
            P("section", "shard", None),
            P("section", "shard", None),
            P("section", "shard", None),
            P(),
        ),
        check_vma=False,
    )
```

```python
import functools
import math

import jax
import jax.numpy as jnp
from jax import lax
from jax.experimental import pallas as pl
from jax.experimental.pallas import tpu as pltpu
from jax.sharding import PartitionSpec as P

MESH = pl.DeviceIdType.MESH
bias_first = 1.0 - 0.9**10
bias_second = 1.0 - 0.99**10
root_second = math.sqrt(bias_second)
LANES = 128
CUTS = (3, 5, 9, 17, 24, 29, 32)
SHIFT = 2
ONE_SHOT = True
PARTS = 2
WIDE = 4


def kernel(
    n_sec, n_y, n_x, cuts,
    g_hbm, p_hbm, m1_hbm, m2_hbm, layer_hbm, valid_hbm, decay_hbm,
    p_v, upd, new1_ref, new2_ref, chosen_ref, total_ref,
    mine, d2d, m1_v, m2_v, r1x, r1y, s1x, s1y, r2x, r2y, xa, ya, xs, ys, tiles, ztiles, layer_ref, valid_ref, decay_ref,
):
    count = len(cuts)
    most = max(n_x, n_y) - 1
    one_shot = ztiles is None
    dma = pltpu.SemaphoreType.DMA
    pl.run_scoped(
        functools.partial(
            body, n_sec, n_y, n_x, cuts, one_shot,
            g_hbm, p_hbm, m1_hbm, m2_hbm, layer_hbm, valid_hbm, decay_hbm,
            p_v, upd, new1_ref, new2_ref, chosen_ref, total_ref,
            mine, d2d, m1_v, m2_v, (r1x, r1y), (s1x, s1y), (r2x, r2y), (xa, ya), (xs, ys), tiles, ztiles,
            layer_ref, valid_ref, decay_ref,
        ),
        load_sem=dma((count, 2)),
        state_sem=dma((6,)),
        pair_send=dma((count, 2)),
        one_send=dma((count, 2, most)),
        two_send=dma((count, 2, most)),
        raw_send=dma((2, most)),
        lent_send=dma((2, 2, most)),
        lent_recv=dma((2, most)),
        t_send=dma((1,)),
        z_send=dma((1,)),
        pair_recv=dma((count, 2)),
        one_recv=dma((count, 2, most)),
        two_recv=dma((count, 2, most)),
        raw_recv=dma((2, most)),
        t_recv=dma((1,)),
        z_recv=dma((1,)),
        told=pltpu.SemaphoreType.REGULAR((2, n_sec - 1)),
        inside=pltpu.SemaphoreType.REGULAR,
        whole=pltpu.SemaphoreType.REGULAR,
        settled=pltpu.SemaphoreType.REGULAR,
    )


def body(
    n_sec, n_y, n_x, cuts, one_shot,
    g_hbm, p_hbm, m1_hbm, m2_hbm, layer_hbm, valid_hbm, decay_hbm,
    p_v, upd, new1_ref, new2_ref, chosen_ref, total_ref,
    mine, d2d, m1_v, m2_v, r1, s1, r2, other, lent, tiles, ztiles, layer_ref, valid_ref, decay_ref,
    load_sem, state_sem, pair_send, one_send, two_send, raw_send, lent_send, lent_recv, t_send, z_send,
    pair_recv, one_recv, two_recv, raw_recv, t_recv, z_recv, told, inside, whole, settled,
):
    rows, cols = p_v.shape
    half = cols // 2
    count = len(cuts)
    n_shard = 2 * n_y * n_x
    sec, me = lax.axis_index("section"), lax.axis_index("shard")
    core = lax.rem(me, 2)
    is_far, is_near = core == 0, core == 1
    x = lax.rem(me // 2, n_x)
    y = me // (2 * n_x)
    blocks = layer_ref.shape[1]
    block_rows = rows // blocks

    def at(yy, xx, cc):
        return (sec, (yy * n_x + xx) * 2 + cc)

    starts = (0,) + cuts[:-1]

    def span(k, d):
        return pl.ds(d * half + starts[k], cuts[k] - starts[k])

    def inner(k):
        return pl.ds(starts[k], cuts[k] - starts[k])

    order = [1, 0, *range(2, count)]
    loads = {}
    for k in order:
        for d in range(2):
            c = pltpu.make_async_copy(
                g_hbm.at[:, :, :, :, span(k, d)], mine.at[:, :, :, :, span(k, d)], load_sem.at[k, d]
            )
            c.start()
            loads[k, d] = c
        if k == 1:
            barrier = pltpu.get_barrier_semaphore()
            beside = at(y, x, 1 - core)
            around = [at(y, lax.rem(x + j, n_x), core) for j in range(1, n_x)]
            around += [at(lax.rem(y + j, n_y), x, core) for j in range(1, n_y)]
            last_sec = n_sec - 1
            up = (jnp.minimum(sec + 1, last_sec), me)
            down = (jnp.maximum(sec - 1, 0), me)
            ends = jnp.where(sec < last_sec, 1, 0) + jnp.where(sec > 0, 1, 0)

            def tell(semaphore):
                for peer in around:
                    pl.semaphore_signal(semaphore, inc=1, device_id=peer, device_id_type=MESH)

                @pl.when(sec < last_sec)
                def _():
                    pl.semaphore_signal(semaphore, inc=1, device_id=up, device_id_type=MESH)

                @pl.when(sec > 0)
                def _():
                    pl.semaphore_signal(semaphore, inc=1, device_id=down, device_id_type=MESH)

            @pl.when(is_near)
            def _():
                tell(barrier)
                pl.semaphore_signal(barrier, inc=1, device_id=beside, device_id_type=MESH)

    states = [
        pltpu.make_async_copy(src, dst, state_sem.at[i])
        for i, (src, dst) in enumerate(
            (
                (layer_hbm, layer_ref), (valid_hbm, valid_ref), (decay_hbm, decay_ref),
                (p_hbm, p_v), (m1_hbm, m1_v), (m2_hbm, m2_v),
            )
        )
    ]
    for s in states:
        s.start()

    @pl.when(is_far)
    def _():
        pl.semaphore_wait(barrier, 1)
        pl.semaphore_signal(inside, inc=1, device_id=beside, device_id_type=MESH)
        for d in range(2):
            other[d][...] = jnp.zeros_like(other[d])

    @pl.when(is_near)
    def _():
        with jax.named_scope("bar1"):
            pl.semaphore_wait(inside, 1)
            pl.semaphore_wait(barrier, len(around) + ends)
        tell(whole)
        pl.semaphore_signal(inside, inc=1, device_id=beside, device_id_type=MESH)

    def meet():
        with jax.named_scope("bar"):

            @pl.when(is_near)
            def _():
                pl.semaphore_wait(whole, len(around) + ends)
                pl.semaphore_signal(settled, inc=1, device_id=beside, device_id_type=MESH)

            @pl.when(is_far)
            def _():
                pl.semaphore_wait(settled, 1)

    def relay(d):
        if 1 < d <= n_sec:

            @pl.when(sec >= d - 1)
            def _():
                pl.semaphore_wait(told.at[0, d - 2], 1)

            @pl.when(sec <= n_sec - d)
            def _():
                pl.semaphore_wait(told.at[1, d - 2], 1)

        if d < n_sec:

            @pl.when((sec >= d - 1) & (sec < last_sec))
            def _():
                pl.semaphore_signal(told.at[0, d - 1], inc=1, device_id=up, device_id_type=MESH)

            @pl.when((sec <= n_sec - d) & (sec > 0))
            def _():
                pl.semaphore_signal(told.at[1, d - 1], inc=1, device_id=down, device_id_type=MESH)

    def place(d, t):
        return (slice(None), t) if d == 0 else (t, slice(None))

    def peer_at(d, t, cc):
        return at(y, t, cc) if d == 0 else at(t, x, cc)

    here = (x, y)
    first_n, second_n = (n_x, n_y), (n_y, n_x)

    def others(d):
        return [(j, lax.rem(here[d] + j, first_n[d])) for j in range(1, first_n[d])]

    def remote(src, dst, send_sem, recv_sem, peer):
        return pltpu.make_async_remote_copy(
            src_ref=src, dst_ref=dst, send_sem=send_sem, recv_sem=recv_sem, device_id=peer, device_id_type=MESH
        )

    def rows_of(d, t, cc, k):
        return mine.at[(*place(d, t), cc, slice(None), span(k, d))]

    ones, raws, lends, crosses, pair, kept = {}, {}, {}, {}, {}, {}
    for d in range(2):
        for k in range(count):
            ones[k, d] = [
                remote(
                    rows_of(d, t, core, k), r1[d].at[j - 1, :, :, inner(k)],
                    one_send.at[k, d, j - 1], one_recv.at[k, d, j - 1], peer_at(d, t, core),
                )
                for j, t in others(d)
            ]
            for group, t in ((pair, slice(None)), (kept, here[d])):
                if group is kept and k not in (0, SHIFT):
                    continue
                spot = place(d, t)
                group[k, d] = remote(
                    rows_of(d, t, 1 - core, k), d2d.at[(*spot, slice(None), span(k, d))],
                    pair_send.at[k, d], pair_recv.at[k, d], at(y, x, 1 - core),
                )
        raws[d] = [
            remote(
                rows_of(d, t, 1 - core, 0), other[d].at[j - 1],
                raw_send.at[d, j - 1], raw_recv.at[d, j - 1], peer_at(d, t, 1 - core),
            )
            for j, t in others(d)
        ]
        lends[d] = [
            remote(
                rows_of(d, t, core, SHIFT), lent[d].at[j - 1],
                lent_send.at[0, d, j - 1], lent_recv.at[d, j - 1], at(y, x, 1 - core),
            )
            for j, t in others(d)
        ]
        crosses[d] = [
            remote(
                rows_of(d, t, 1 - core, SHIFT), r1[d].at[j - 1, :, :, inner(SHIFT)],
                lent_send.at[1, d, j - 1], one_recv.at[SHIFT, d, j - 1], peer_at(d, t, 1 - core),
            )
            for j, t in others(d)
        ]

    def send_pair(k, d):
        if k:
            with jax.named_scope(f"ldw{k}{d}"):
                loads[k, d].wait()
        if k == 0:

            @pl.when(is_far)
            def _():
                loads[k, d].wait()
                kept[k, d].start()

            @pl.when(is_near)
            def _():
                pair[k, d].start()
        elif k == SHIFT:

            @pl.when(is_far)
            def _():
                for c in (pair[k, d], *lends[d]):
                    c.start()

            @pl.when(is_near)
            def _():
                kept[k, d].start()
        else:
            pair[k, d].start()

    def add_pair(yy, xx, cut):
        total = mine[yy, xx, core, :, cut].astype(jnp.float32) + d2d[yy, xx, :, cut].astype(jnp.float32)
        mine[yy, xx, core, :, cut] = total.astype(jnp.bfloat16)

    def add_all(cut):
        def add_one(i, carry):
            add_pair(i // n_x, lax.rem(i, n_x), cut)
            return carry

        lax.fori_loop(0, n_y * n_x, add_one, 0)

    def add_kept(d, cut):
        for i in range(second_n[d]):
            add_pair(i if d == 0 else y, x if d == 0 else i, cut)

    def send_one(k, d):
        cut = span(k, d)
        if k == 0:

            @pl.when(is_near)
            def _():
                kept[k, d].wait_recv()
                add_kept(d, cut)

            @pl.when(is_far)
            def _():
                pair[k, d].wait_recv()
                add_all(cut)
                for c in ones[k, d]:
                    c.start()

        elif k == SHIFT:

            @pl.when(is_near)
            def _():
                pair[k, d].wait_recv()
                for c in lends[d]:
                    c.wait_recv()
                add_all(cut)
                for c in ones[k, d]:
                    c.start()
                for j, t in others(d):
                    for i in range(second_n[d]):
                        yy, xx = (i, t) if d == 0 else (t, i)
                        total = mine[yy, xx, 1 - core, :, cut].astype(jnp.float32)
                        total += lent[d][j - 1, i].astype(jnp.float32)
                        mine[yy, xx, 1 - core, :, cut] = total.astype(jnp.bfloat16)
                for c in crosses[d]:
                    c.start()

            @pl.when(is_far)
            def _():
                kept[k, d].wait_recv()
                add_kept(d, cut)
        else:
            with jax.named_scope(f"pairw{k}{d}"):
                pair[k, d].wait_recv()
            add_all(cut)
            for c in ones[k, d]:
                c.start()

    @pl.when(is_near)
    def _():
        for d in range(2):
            loads[0, d].wait()
            for c in ones[0, d]:
                c.start()

    ahead = 3
    for i, k in enumerate(order[: 1 + ahead]):
        if i == 2:

            @pl.when(is_far)
            def _():
                pl.semaphore_wait(inside, 1)
                for d in range(2):
                    for c in raws[d]:
                        c.start()

            meet()
        for d in range(2):
            send_pair(k, d)
    for i, k in enumerate(order):
        for d in range(2):
            send_one(k, d)
        if i + 1 + ahead < count:
            for d in range(2):
                send_pair(order[i + 1 + ahead], d)

    def partial(k, d, t, cut, near_cut, raw_cut):
        yy, xx = (t, x) if d == 0 else (y, t)
        total = mine[yy, xx, core, :, cut].astype(jnp.float32)
        for i in range(first_n[d] - 1):
            total += r1[d][i, t, :, near_cut].astype(jnp.float32)
            if k == 0:
                total += other[d][i, t, :, raw_cut].astype(jnp.float32)
        return total

    def by_block(scalars):
        return jnp.concatenate([jnp.full((block_rows, LANES), s) for s in scalars], axis=0)

    for s in states:
        s.wait()
    layers = [layer_ref[0, b] for b in range(blocks)]
    lives = [valid_ref[0, b] for b in range(blocks)]
    row_decay = by_block([decay_ref[layer] for layer in layers])
    row_live = by_block([jnp.where(v > 0, 1.0, 0.0).astype(jnp.float32) for v in lives]) > 0.5
    n_layer = decay_ref.shape[0]
    lane = lax.broadcasted_iota(jnp.int32, (1, LANES), 1)

    def by_layer(values, offset):
        terms = []
        for b in range(blocks):
            chosen = jnp.where(lives[b] > 0, layers[b] + offset, -1)
            block = values[b * block_rows : (b + 1) * block_rows]
            terms.append(jnp.where(lane == chosen, jnp.sum(block, axis=1, keepdims=True), 0.0))
        return jnp.sum(sum(terms[1:], terms[0]), axis=0, keepdims=True)

    def weigh(i, wsum):
        weights = p_v[:, pl.ds(pl.multiple_of(i * LANES, LANES), LANES)].astype(jnp.float32)
        return wsum + weights * weights

    zero = jnp.zeros((rows, LANES), jnp.float32)
    chosen_ref[...] = jnp.concatenate(
        [
            jnp.broadcast_to(jnp.where((lane == layers[b]) & (lives[b] > 0), 0.1, 0.0), (block_rows, LANES))
            for b in range(blocks)
        ],
        axis=0,
    )
    weight_line = by_layer(lax.fori_loop(0, cols // LANES, weigh, zero, unroll=2), 0)

    twos = {}
    for k in range(count):
        for d in range(2):
            with jax.named_scope(f"onew{k}{d}"):
                for c in ones[k, d]:
                    c.wait_recv()
                if k == 0:

                    @pl.when(is_near)
                    def _(d=d):
                        for c in raws[d]:
                            c.wait_recv()

            group = []
            for j in range(1, second_n[d]):
                at_hand = y if d == 0 else x
                t = lax.rem(at_hand + j, second_n[d])
                total = partial(k, d, t, span(k, d), inner(k), slice(None))
                s1[d][j - 1, :, inner(k)] = total.astype(jnp.bfloat16)
                c = pltpu.make_async_remote_copy(
                    src_ref=s1[d].at[j - 1, :, inner(k)], dst_ref=r2[d].at[j - 1, :, inner(k)],
                    send_sem=two_send.at[k, d, j - 1], recv_sem=two_recv.at[k, d, j - 1],
                    device_id=peer_at(1 - d, t, core), device_id_type=MESH,
                )
                c.start()
                group.append(c)
            twos[k, d] = group
        if 0 < k <= n_sec:
            relay(k)
    for k in range(count, n_sec + 1):
        relay(k)

    for d in range(2):
        for k in range(count):
            if k not in (0, SHIFT):
                pair[k, d].wait_send()

        @pl.when(is_near)
        def _(d=d):
            for c in (pair[0, d], kept[SHIFT, d], *ones[SHIFT, d], *crosses[d]):
                c.wait_send()

        @pl.when(is_far)
        def _(d=d):
            for c in (kept[0, d], pair[SHIFT, d], *lends[d], *raws[d]):
                c.wait_send()

    def lanes(start):
        return pl.ds(start if isinstance(start, int) else pl.multiple_of(start, LANES), LANES)

    usum = zero
    for k in range(count):
        for d in range(2):
            with jax.named_scope(f"twow{k}{d}"):
                for c in twos[k, d]:
                    c.wait_recv()

            def update_piece(i, usum, k=k, d=d):
                raw_cut, near_cut, cut = (lanes(base + i * LANES) for base in (0, starts[k], d * half + starts[k]))
                grad = partial(k, d, y if d == 0 else x, cut, near_cut, raw_cut)
                for j in range(second_n[d] - 1):
                    grad += r2[d][j, :, near_cut].astype(jnp.float32)
                weights = p_v[:, cut].astype(jnp.float32)
                old1, old2 = m1_v[:, cut], m2_v[:, cut]
                tenth = 0.1 * grad
                first = 0.9 * old1 + tenth
                second = 0.99 * old2 + tenth * tenth
                root = second * lax.rsqrt(second)
                update = first * (root_second / bias_first) / (root + 1e-06 * root_second) + row_decay * weights
                upd[:, cut] = update
                new1_ref[:, cut] = jnp.where(row_live, first, old1)
                new2_ref[:, cut] = jnp.where(row_live, second, old2)
                return usum + update * update

            n = (cuts[k] - starts[k]) // LANES

            def update_block(i, usum):
                for u in range(WIDE):
                    usum = update_piece(i * WIDE + u, usum)
                return usum

            with jax.named_scope(f"upd{k}{d}"):
                usum = lax.fori_loop(0, n // WIDE, update_block, usum)
                for i in range(n // WIDE * WIDE, n):
                    usum = update_piece(i, usum)

    line = weight_line + by_layer(usum, n_layer)

    def all_sum(line, slots, send_sem, recv_sem, index, peers, sent):
        slots[index] = line
        for peer in peers:
            pltpu.make_async_remote_copy(
                src_ref=slots.at[index], dst_ref=slots.at[index],
                send_sem=send_sem.at[0], recv_sem=recv_sem.at[0],
                device_id=peer, device_id_type=MESH,
            ).start()
        whole = slots.at[pl.ds(0, len(peers))]
        both = pltpu.make_async_remote_copy(
            src_ref=whole, dst_ref=whole, send_sem=send_sem.at[0], recv_sem=recv_sem.at[0],
            device_id=peers[0], device_id_type=MESH,
        )
        if sent:
            with jax.named_scope("endw"):
                for c in sent:
                    c.wait_send()
        with jax.named_scope("allw"):
            both.wait_recv()
        terms = [slots[j] for j in range(len(peers) + 1)]
        while len(terms) > 1:
            terms = [sum(terms[i + 1 : i + 2], terms[i]) for i in range(0, len(terms), 2)]
        return terms[0], both

    groups = (*(ones[k, d] for k in range(count) if k != SHIFT for d in range(2)), *twos.values())
    sent = [c for group in groups for c in group]
    if one_shot:
        every = [
            (i + jnp.where(i >= sec, 1, 0), j) for i in range(n_sec - 1) for j in range(n_shard)
        ] + [(sec, lax.rem(me + j, n_shard)) for j in range(1, n_shard)]
        line, last = all_sum(line, tiles, t_send, t_recv, sec * n_shard + me, every, sent)
        sends = [last]
    else:
        shard_peers = [(sec, lax.rem(me + j, n_shard)) for j in range(1, n_shard)]
        sec_peers = [(lax.rem(sec + j, n_sec), me) for j in range(1, n_sec)]
        line, last = all_sum(line, tiles, t_send, t_recv, me, shard_peers, sent)
        line, zlast = all_sum(line, ztiles, z_send, z_recv, sec, sec_peers, [])
        sends = [last, zlast]
    total_ref[...] = line
    for c in sends:
        c.wait_send()


def finish(
    parts, p_v, upd, new1_v, new2_v, chosen_v, total_v, newp_hbm, new1_hbm, new2_hbm, ratio_hbm, newp_v, ratio_v, sem
):
    cols = p_v.shape[1]
    width = cols // parts
    copies = []
    for k in range(parts):
        span = pl.ds(k * width, width)
        for i, (src, dst) in enumerate(((new1_v, new1_hbm), (new2_v, new2_hbm))):
            copies.append(pltpu.make_async_copy(src.at[:, span], dst.at[:, span], sem.at[1 + i * parts + k]))
    for c in copies:
        c.start()
    total = total_v[...]
    n_layer = ratio_v.shape[0]
    ratios = jnp.sqrt(total / (pltpu.roll(total, LANES - n_layer, 1) + 1.0))
    ratios = jnp.where(lax.broadcasted_iota(jnp.int32, ratios.shape, 1) < n_layer, ratios, 0.0)
    row_step = jnp.broadcast_to(jnp.sum(chosen_v[...] * ratios, axis=1, keepdims=True), chosen_v.shape)
    ratio_v[...] = ratios[0, :n_layer]
    copies.append(pltpu.make_async_copy(ratio_v, ratio_hbm, sem.at[0]))
    copies[-1].start()

    for k in range(parts):
        def step_piece(i, carry, k=k):
            outer = pl.ds(pl.multiple_of(k * width + i * LANES, LANES), LANES)
            stepped = p_v[:, outer].astype(jnp.float32) - row_step * upd[:, outer]
            newp_v[:, outer] = stepped.astype(jnp.bfloat16)
            return carry

        lax.fori_loop(0, width // LANES, step_piece, 0, unroll=4)
        span = pl.ds(k * width, width)
        c = pltpu.make_async_copy(newp_v.at[:, span], newp_hbm.at[:, span], sem.at[1 + 2 * parts + k])
        c.start()
        copies.append(c)
    for c in copies:
        c.wait()


def shards(grad_parts, params, moment_first, moment_second, block_layer, block_valid, decay):
    n_sec, n_shard = lax.axis_size("section"), lax.axis_size("shard")
    chips = n_shard // 2
    n_y = max(d for d in range(1, math.isqrt(chips) + 1) if chips % d == 0)
    n_x = chips // n_y
    rows, cols = params.shape[1:]
    n_layer = decay.shape[0]
    half = cols // 2
    cuts = tuple(half // LANES * c // CUTS[-1] * LANES for c in CUTS)
    bf16, f32 = jnp.bfloat16, jnp.float32
    dma = pltpu.SemaphoreType.DMA
    one_shot = ONE_SHOT and n_shard * n_sec <= 32
    n_lines = n_shard * n_sec if one_shot else n_shard
    grads = grad_parts.reshape(n_y, n_x, 2, rows, cols)
    any_spec = pl.BlockSpec(memory_space=pltpu.HBM)
    vmem = pl.BlockSpec(memory_space=pltpu.VMEM)
    held = pl.pallas_call(
        functools.partial(kernel, n_sec, n_y, n_x, cuts),
        out_shape=(
            pltpu.VMEM((rows, cols), bf16),
            pltpu.VMEM((rows, cols), f32),
            pltpu.VMEM((rows, cols), f32),
            pltpu.VMEM((rows, cols), f32),
            pltpu.VMEM((rows, LANES), f32),
            pltpu.VMEM((1, LANES), f32),
        ),
        in_specs=[any_spec] * 7,
        out_specs=(vmem,) * 6,
        scratch_shapes=[
            pltpu.VMEM((n_y, n_x, 2, rows, cols), bf16),
            pltpu.VMEM((n_y, n_x, rows, cols), bf16),
            pltpu.VMEM((rows, cols), f32),
            pltpu.VMEM((rows, cols), f32),
            pltpu.VMEM((n_x - 1, n_y, rows, half), bf16),
            pltpu.VMEM((n_y - 1, n_x, rows, half), bf16),
            pltpu.VMEM((n_y - 1, rows, half), bf16),
            pltpu.VMEM((n_x - 1, rows, half), bf16),
            pltpu.VMEM((n_y - 1, rows, half), bf16),
            pltpu.VMEM((n_x - 1, rows, half), bf16),
            pltpu.VMEM((n_x - 1, n_y, rows, cuts[0]), bf16),
            pltpu.VMEM((n_y - 1, n_x, rows, cuts[0]), bf16),
            pltpu.VMEM((n_x - 1, n_y, rows, cuts[SHIFT] - cuts[SHIFT - 1]), bf16),
            pltpu.VMEM((n_y - 1, n_x, rows, cuts[SHIFT] - cuts[SHIFT - 1]), bf16),
            pltpu.VMEM((n_lines, 1, LANES), f32),
            None if one_shot else pltpu.VMEM((n_sec, 1, LANES), f32),
            pltpu.SMEM(block_layer.shape, jnp.int32),
            pltpu.SMEM(block_valid.shape, jnp.int32),
            pltpu.SMEM(decay.shape, f32),
        ],
        compiler_params=pltpu.CompilerParams(
            collective_id=0, has_side_effects=True, vmem_limit_bytes=56 * 1024 * 1024
        ),
    )(grads, params[0], moment_first[0], moment_second[0], block_layer, block_valid, decay)
    out = pl.pallas_call(
        functools.partial(finish, PARTS),
        out_shape=(
            jax.ShapeDtypeStruct((rows, cols), bf16),
            jax.ShapeDtypeStruct((rows, cols), f32),
            jax.ShapeDtypeStruct((rows, cols), f32),
            jax.ShapeDtypeStruct((n_layer,), f32),
        ),
        in_specs=[vmem] * 6,
        out_specs=(any_spec,) * 4,
        scratch_shapes=[pltpu.VMEM((rows, cols), bf16), pltpu.VMEM((n_layer,), f32), dma((1 + 3 * PARTS,))],
        compiler_params=pltpu.CompilerParams(vmem_limit_bytes=8 * 1024 * 1024),
    )(*held)
    return (out[0][None], out[1][None], out[2][None], out[3])


def solution(mesh):
    placed = (
        P("section", "shard", None, None),
        P("section", "shard", None),
        P("section", "shard", None),
        P("section", "shard", None),
        P("section", "shard"),
        P("section", "shard"),
        P(),
    )
    return jax.shard_map(
        shards,
        mesh=mesh,
        in_specs=placed,
        out_specs=(
            P("section", "shard", None),
            P("section", "shard", None),
            P("section", "shard", None),
            P(),
        ),
        check_vma=False,
    )
```

```python
import functools
import math

import jax
import jax.numpy as jnp
from jax import lax
from jax.experimental import pallas as pl
from jax.experimental.pallas import tpu as pltpu
from jax.sharding import PartitionSpec as P

MESH = pl.DeviceIdType.MESH
bias_first = 1.0 - 0.9**10
bias_second = 1.0 - 0.99**10
root_second = math.sqrt(bias_second)
LANES = 128
CUTS = (3, 5, 9, 17, 24, 28, 31, 32)
SHIFT = 2
ONE_SHOT = True
PARTS = 2
WIDE = 4


def kernel(
    n_sec, n_y, n_x, cuts,
    g_hbm, p_hbm, m1_hbm, m2_hbm, layer_hbm, valid_hbm, decay_hbm,
    p_v, upd, new1_ref, new2_ref, chosen_ref, total_ref,
    mine, d2d, m1_v, m2_v, r1x, r1y, s1x, s1y, r2x, r2y, xa, ya, xs, ys, tiles, ztiles, layer_ref, valid_ref, decay_ref,
):
    count = len(cuts)
    most = max(n_x, n_y) - 1
    one_shot = ztiles is None
    dma = pltpu.SemaphoreType.DMA
    pl.run_scoped(
        functools.partial(
            body, n_sec, n_y, n_x, cuts, one_shot,
            g_hbm, p_hbm, m1_hbm, m2_hbm, layer_hbm, valid_hbm, decay_hbm,
            p_v, upd, new1_ref, new2_ref, chosen_ref, total_ref,
            mine, d2d, m1_v, m2_v, (r1x, r1y), (s1x, s1y), (r2x, r2y), (xa, ya), (xs, ys), tiles, ztiles,
            layer_ref, valid_ref, decay_ref,
        ),
        load_sem=dma((count, 2)),
        state_sem=dma((6,)),
        pair_send=dma((count, 2)),
        one_send=dma((count, 2, most)),
        two_send=dma((count, 2, most)),
        raw_send=dma((2, most)),
        lent_send=dma((2, 2, most)),
        lent_recv=dma((2, most)),
        t_send=dma((1,)),
        z_send=dma((1,)),
        pair_recv=dma((count, 2)),
        one_recv=dma((count, 2, most)),
        two_recv=dma((count, 2, most)),
        raw_recv=dma((2, most)),
        t_recv=dma((1,)),
        z_recv=dma((1,)),
        told=pltpu.SemaphoreType.REGULAR((2, n_sec - 1)),
        inside=pltpu.SemaphoreType.REGULAR,
        whole=pltpu.SemaphoreType.REGULAR,
        settled=pltpu.SemaphoreType.REGULAR,
    )


def body(
    n_sec, n_y, n_x, cuts, one_shot,
    g_hbm, p_hbm, m1_hbm, m2_hbm, layer_hbm, valid_hbm, decay_hbm,
    p_v, upd, new1_ref, new2_ref, chosen_ref, total_ref,
    mine, d2d, m1_v, m2_v, r1, s1, r2, other, lent, tiles, ztiles, layer_ref, valid_ref, decay_ref,
    load_sem, state_sem, pair_send, one_send, two_send, raw_send, lent_send, lent_recv, t_send, z_send,
    pair_recv, one_recv, two_recv, raw_recv, t_recv, z_recv, told, inside, whole, settled,
):
    rows, cols = p_v.shape
    half = cols // 2
    count = len(cuts)
    n_shard = 2 * n_y * n_x
    sec, me = lax.axis_index("section"), lax.axis_index("shard")
    core = lax.rem(me, 2)
    is_far, is_near = core == 0, core == 1
    x = lax.rem(me // 2, n_x)
    y = me // (2 * n_x)
    blocks = layer_ref.shape[1]
    block_rows = rows // blocks

    def at(yy, xx, cc):
        return (sec, (yy * n_x + xx) * 2 + cc)

    starts = (0,) + cuts[:-1]

    def span(k, d):
        return pl.ds(d * half + starts[k], cuts[k] - starts[k])

    def inner(k):
        return pl.ds(starts[k], cuts[k] - starts[k])

    order = [1, 0, *range(2, count)]
    loads = {}
    for k in order:
        for d in range(2):
            c = pltpu.make_async_copy(
                g_hbm.at[:, :, :, :, span(k, d)], mine.at[:, :, :, :, span(k, d)], load_sem.at[k, d]
            )
            c.start()
            loads[k, d] = c
        if k == 1:
            barrier = pltpu.get_barrier_semaphore()
            beside = at(y, x, 1 - core)
            around = [at(y, lax.rem(x + j, n_x), core) for j in range(1, n_x)]
            around += [at(lax.rem(y + j, n_y), x, core) for j in range(1, n_y)]
            last_sec = n_sec - 1
            up = (jnp.minimum(sec + 1, last_sec), me)
            down = (jnp.maximum(sec - 1, 0), me)
            ends = jnp.where(sec < last_sec, 1, 0) + jnp.where(sec > 0, 1, 0)

            def tell(semaphore):
                for peer in around:
                    pl.semaphore_signal(semaphore, inc=1, device_id=peer, device_id_type=MESH)

                @pl.when(sec < last_sec)
                def _():
                    pl.semaphore_signal(semaphore, inc=1, device_id=up, device_id_type=MESH)

                @pl.when(sec > 0)
                def _():
                    pl.semaphore_signal(semaphore, inc=1, device_id=down, device_id_type=MESH)

            @pl.when(is_near)
            def _():
                tell(barrier)
                pl.semaphore_signal(barrier, inc=1, device_id=beside, device_id_type=MESH)

    states = [
        pltpu.make_async_copy(src, dst, state_sem.at[i])
        for i, (src, dst) in enumerate(
            (
                (layer_hbm, layer_ref), (valid_hbm, valid_ref), (decay_hbm, decay_ref),
                (p_hbm, p_v), (m1_hbm, m1_v), (m2_hbm, m2_v),
            )
        )
    ]
    for s in states:
        s.start()

    @pl.when(is_far)
    def _():
        pl.semaphore_wait(barrier, 1)
        pl.semaphore_signal(inside, inc=1, device_id=beside, device_id_type=MESH)
        for d in range(2):
            other[d][...] = jnp.zeros_like(other[d])

    @pl.when(is_near)
    def _():
        with jax.named_scope("bar1"):
            pl.semaphore_wait(inside, 1)
            pl.semaphore_wait(barrier, len(around) + ends)
        tell(whole)
        pl.semaphore_signal(inside, inc=1, device_id=beside, device_id_type=MESH)

    def meet():
        with jax.named_scope("bar"):

            @pl.when(is_near)
            def _():
                pl.semaphore_wait(whole, len(around) + ends)
                pl.semaphore_signal(settled, inc=1, device_id=beside, device_id_type=MESH)

            @pl.when(is_far)
            def _():
                pl.semaphore_wait(settled, 1)

    def relay(d):
        if 1 < d <= n_sec:

            @pl.when(sec >= d - 1)
            def _():
                pl.semaphore_wait(told.at[0, d - 2], 1)

            @pl.when(sec <= n_sec - d)
            def _():
                pl.semaphore_wait(told.at[1, d - 2], 1)

        if d < n_sec:

            @pl.when((sec >= d - 1) & (sec < last_sec))
            def _():
                pl.semaphore_signal(told.at[0, d - 1], inc=1, device_id=up, device_id_type=MESH)

            @pl.when((sec <= n_sec - d) & (sec > 0))
            def _():
                pl.semaphore_signal(told.at[1, d - 1], inc=1, device_id=down, device_id_type=MESH)

    def place(d, t):
        return (slice(None), t) if d == 0 else (t, slice(None))

    def peer_at(d, t, cc):
        return at(y, t, cc) if d == 0 else at(t, x, cc)

    here = (x, y)
    first_n, second_n = (n_x, n_y), (n_y, n_x)

    def others(d):
        return [(j, lax.rem(here[d] + j, first_n[d])) for j in range(1, first_n[d])]

    def remote(src, dst, send_sem, recv_sem, peer):
        return pltpu.make_async_remote_copy(
            src_ref=src, dst_ref=dst, send_sem=send_sem, recv_sem=recv_sem, device_id=peer, device_id_type=MESH
        )

    def rows_of(d, t, cc, k):
        return mine.at[(*place(d, t), cc, slice(None), span(k, d))]

    ones, raws, lends, crosses, pair, kept = {}, {}, {}, {}, {}, {}
    for d in range(2):
        for k in range(count):
            ones[k, d] = [
                remote(
                    rows_of(d, t, core, k), r1[d].at[j - 1, :, :, inner(k)],
                    one_send.at[k, d, j - 1], one_recv.at[k, d, j - 1], peer_at(d, t, core),
                )
                for j, t in others(d)
            ]
            for group, t in ((pair, slice(None)), (kept, here[d])):
                if group is kept and k not in (0, SHIFT):
                    continue
                spot = place(d, t)
                group[k, d] = remote(
                    rows_of(d, t, 1 - core, k), d2d.at[(*spot, slice(None), span(k, d))],
                    pair_send.at[k, d], pair_recv.at[k, d], at(y, x, 1 - core),
                )
        raws[d] = [
            remote(
                rows_of(d, t, 1 - core, 0), other[d].at[j - 1],
                raw_send.at[d, j - 1], raw_recv.at[d, j - 1], peer_at(d, t, 1 - core),
            )
            for j, t in others(d)
        ]
        lends[d] = [
            remote(
                rows_of(d, t, core, SHIFT), lent[d].at[j - 1],
                lent_send.at[0, d, j - 1], lent_recv.at[d, j - 1], at(y, x, 1 - core),
            )
            for j, t in others(d)
        ]
        crosses[d] = [
            remote(
                rows_of(d, t, 1 - core, SHIFT), r1[d].at[j - 1, :, :, inner(SHIFT)],
                lent_send.at[1, d, j - 1], one_recv.at[SHIFT, d, j - 1], peer_at(d, t, 1 - core),
            )
            for j, t in others(d)
        ]

    def send_pair(k, d):
        if k:
            with jax.named_scope(f"ldw{k}{d}"):
                loads[k, d].wait()
        if k == 0:

            @pl.when(is_far)
            def _():
                loads[k, d].wait()
                kept[k, d].start()

            @pl.when(is_near)
            def _():
                pair[k, d].start()
        elif k == SHIFT:

            @pl.when(is_far)
            def _():
                for c in (pair[k, d], *lends[d]):
                    c.start()

            @pl.when(is_near)
            def _():
                kept[k, d].start()
        else:
            pair[k, d].start()

    def add_pair(yy, xx, cut):
        total = mine[yy, xx, core, :, cut].astype(jnp.float32) + d2d[yy, xx, :, cut].astype(jnp.float32)
        mine[yy, xx, core, :, cut] = total.astype(jnp.bfloat16)

    def add_all(cut):
        def add_one(i, carry):
            add_pair(i // n_x, lax.rem(i, n_x), cut)
            return carry

        lax.fori_loop(0, n_y * n_x, add_one, 0)

    def add_kept(d, cut):
        for i in range(second_n[d]):
            add_pair(i if d == 0 else y, x if d == 0 else i, cut)

    def send_one(k, d):
        cut = span(k, d)
        if k == 0:

            @pl.when(is_near)
            def _():
                kept[k, d].wait_recv()
                add_kept(d, cut)

            @pl.when(is_far)
            def _():
                pair[k, d].wait_recv()
                add_all(cut)
                for c in ones[k, d]:
                    c.start()

        elif k == SHIFT:

            @pl.when(is_near)
            def _():
                pair[k, d].wait_recv()
                for c in lends[d]:
                    c.wait_recv()
                add_all(cut)
                for c in ones[k, d]:
                    c.start()
                for j, t in others(d):
                    for i in range(second_n[d]):
                        yy, xx = (i, t) if d == 0 else (t, i)
                        total = mine[yy, xx, 1 - core, :, cut].astype(jnp.float32)
                        total += lent[d][j - 1, i].astype(jnp.float32)
                        mine[yy, xx, 1 - core, :, cut] = total.astype(jnp.bfloat16)
                for c in crosses[d]:
                    c.start()

            @pl.when(is_far)
            def _():
                kept[k, d].wait_recv()
                add_kept(d, cut)
        else:
            with jax.named_scope(f"pairw{k}{d}"):
                pair[k, d].wait_recv()
            add_all(cut)
            for c in ones[k, d]:
                c.start()

    @pl.when(is_near)
    def _():
        for d in range(2):
            loads[0, d].wait()
            for c in ones[0, d]:
                c.start()

    ahead = 4
    behind = 2

    def push(which, i):
        if 3 <= i < count:

            @pl.when(which)
            def _():
                for d in range(2):
                    send_pair(order[i], d)

    for i, k in enumerate(order[:3]):
        if i == 2:

            @pl.when(is_far)
            def _():
                pl.semaphore_wait(inside, 1)
                for d in range(2):
                    for c in raws[d]:
                        c.start()

            meet()
        for d in range(2):
            send_pair(k, d)
    for i in range(3, 1 + ahead):
        push(is_near, i)
    for i in range(3, 1 + behind):
        push(is_far, i)
    for i, k in enumerate(order):
        for d in range(2):
            send_one(k, d)
        push(is_near, i + 1 + ahead)
        push(is_far, i + 1 + behind)

    def partial(k, d, t, cut, near_cut, raw_cut):
        yy, xx = (t, x) if d == 0 else (y, t)
        total = mine[yy, xx, core, :, cut].astype(jnp.float32)
        for i in range(first_n[d] - 1):
            total += r1[d][i, t, :, near_cut].astype(jnp.float32)
            if k == 0:
                total += other[d][i, t, :, raw_cut].astype(jnp.float32)
        return total

    def by_block(scalars):
        return jnp.concatenate([jnp.full((block_rows, LANES), s) for s in scalars], axis=0)

    for s in states:
        s.wait()
    layers = [layer_ref[0, b] for b in range(blocks)]
    lives = [valid_ref[0, b] for b in range(blocks)]
    row_decay = by_block([decay_ref[layer] for layer in layers])
    row_live = by_block([jnp.where(v > 0, 1.0, 0.0).astype(jnp.float32) for v in lives]) > 0.5
    n_layer = decay_ref.shape[0]
    lane = lax.broadcasted_iota(jnp.int32, (1, LANES), 1)

    def by_layer(values, offset):
        terms = []
        for b in range(blocks):
            chosen = jnp.where(lives[b] > 0, layers[b] + offset, -1)
            block = values[b * block_rows : (b + 1) * block_rows]
            terms.append(jnp.where(lane == chosen, jnp.sum(block, axis=1, keepdims=True), 0.0))
        return jnp.sum(sum(terms[1:], terms[0]), axis=0, keepdims=True)

    def weigh(i, wsum):
        weights = p_v[:, pl.ds(pl.multiple_of(i * LANES, LANES), LANES)].astype(jnp.float32)
        return wsum + weights * weights

    zero = jnp.zeros((rows, LANES), jnp.float32)
    chosen_ref[...] = jnp.concatenate(
        [
            jnp.broadcast_to(jnp.where((lane == layers[b]) & (lives[b] > 0), 0.1, 0.0), (block_rows, LANES))
            for b in range(blocks)
        ],
        axis=0,
    )
    weight_line = by_layer(lax.fori_loop(0, cols // LANES, weigh, zero, unroll=2), 0)

    twos = {}
    for k in range(count):
        for d in range(2):
            with jax.named_scope(f"onew{k}{d}"):
                for c in ones[k, d]:
                    c.wait_recv()
                if k == 0:

                    @pl.when(is_near)
                    def _(d=d):
                        for c in raws[d]:
                            c.wait_recv()

            group = []
            for j in range(1, second_n[d]):
                at_hand = y if d == 0 else x
                t = lax.rem(at_hand + j, second_n[d])
                total = partial(k, d, t, span(k, d), inner(k), slice(None))
                s1[d][j - 1, :, inner(k)] = total.astype(jnp.bfloat16)
                c = pltpu.make_async_remote_copy(
                    src_ref=s1[d].at[j - 1, :, inner(k)], dst_ref=r2[d].at[j - 1, :, inner(k)],
                    send_sem=two_send.at[k, d, j - 1], recv_sem=two_recv.at[k, d, j - 1],
                    device_id=peer_at(1 - d, t, core), device_id_type=MESH,
                )
                c.start()
                group.append(c)
            twos[k, d] = group
        if 0 < k <= n_sec:
            relay(k)
    for k in range(count, n_sec + 1):
        relay(k)

    for d in range(2):
        for k in range(count):
            if k not in (0, SHIFT):
                pair[k, d].wait_send()

        @pl.when(is_near)
        def _(d=d):
            for c in (pair[0, d], kept[SHIFT, d], *ones[SHIFT, d], *crosses[d]):
                c.wait_send()

        @pl.when(is_far)
        def _(d=d):
            for c in (kept[0, d], pair[SHIFT, d], *lends[d], *raws[d]):
                c.wait_send()

    def lanes(start):
        return pl.ds(start if isinstance(start, int) else pl.multiple_of(start, LANES), LANES)

    usum = zero
    for k in range(count):
        for d in range(2):
            with jax.named_scope(f"twow{k}{d}"):
                for c in twos[k, d]:
                    c.wait_recv()

            def update_piece(i, usum, k=k, d=d):
                raw_cut, near_cut, cut = (lanes(base + i * LANES) for base in (0, starts[k], d * half + starts[k]))
                grad = partial(k, d, y if d == 0 else x, cut, near_cut, raw_cut)
                for j in range(second_n[d] - 1):
                    grad += r2[d][j, :, near_cut].astype(jnp.float32)
                weights = p_v[:, cut].astype(jnp.float32)
                old1, old2 = m1_v[:, cut], m2_v[:, cut]
                tenth = 0.1 * grad
                first = 0.9 * old1 + tenth
                second = 0.99 * old2 + tenth * tenth
                root = second * lax.rsqrt(second)
                update = first * (root_second / bias_first) / (root + 1e-06 * root_second) + row_decay * weights
                upd[:, cut] = update
                new1_ref[:, cut] = jnp.where(row_live, first, old1)
                new2_ref[:, cut] = jnp.where(row_live, second, old2)
                return usum + update * update

            n = (cuts[k] - starts[k]) // LANES

            def update_block(i, usum):
                for u in range(WIDE):
                    usum = update_piece(i * WIDE + u, usum)
                return usum

            with jax.named_scope(f"upd{k}{d}"):
                usum = lax.fori_loop(0, n // WIDE, update_block, usum)
                for i in range(n // WIDE * WIDE, n):
                    usum = update_piece(i, usum)

    line = weight_line + by_layer(usum, n_layer)

    def all_sum(line, slots, send_sem, recv_sem, index, peers, sent):
        slots[index] = line
        for peer in peers:
            pltpu.make_async_remote_copy(
                src_ref=slots.at[index], dst_ref=slots.at[index],
                send_sem=send_sem.at[0], recv_sem=recv_sem.at[0],
                device_id=peer, device_id_type=MESH,
            ).start()
        whole = slots.at[pl.ds(0, len(peers))]
        both = pltpu.make_async_remote_copy(
            src_ref=whole, dst_ref=whole, send_sem=send_sem.at[0], recv_sem=recv_sem.at[0],
            device_id=peers[0], device_id_type=MESH,
        )
        if sent:
            with jax.named_scope("endw"):
                for c in sent:
                    c.wait_send()
        with jax.named_scope("allw"):
            both.wait_recv()
        terms = [slots[j] for j in range(len(peers) + 1)]
        while len(terms) > 1:
            terms = [sum(terms[i + 1 : i + 2], terms[i]) for i in range(0, len(terms), 2)]
        return terms[0], both

    groups = (*(ones[k, d] for k in range(count) if k != SHIFT for d in range(2)), *twos.values())
    sent = [c for group in groups for c in group]
    if one_shot:
        every = [
            (i + jnp.where(i >= sec, 1, 0), j) for i in range(n_sec - 1) for j in range(n_shard)
        ] + [(sec, lax.rem(me + j, n_shard)) for j in range(1, n_shard)]
        line, last = all_sum(line, tiles, t_send, t_recv, sec * n_shard + me, every, sent)
        sends = [last]
    else:
        shard_peers = [(sec, lax.rem(me + j, n_shard)) for j in range(1, n_shard)]
        sec_peers = [(lax.rem(sec + j, n_sec), me) for j in range(1, n_sec)]
        line, last = all_sum(line, tiles, t_send, t_recv, me, shard_peers, sent)
        line, zlast = all_sum(line, ztiles, z_send, z_recv, sec, sec_peers, [])
        sends = [last, zlast]
    total_ref[...] = line
    for c in sends:
        c.wait_send()


def finish(
    parts, p_v, upd, new1_v, new2_v, chosen_v, total_v, newp_hbm, new1_hbm, new2_hbm, ratio_hbm, newp_v, ratio_v, sem
):
    cols = p_v.shape[1]
    width = cols // parts
    copies = []
    for k in range(parts):
        span = pl.ds(k * width, width)
        for i, (src, dst) in enumerate(((new1_v, new1_hbm), (new2_v, new2_hbm))):
            copies.append(pltpu.make_async_copy(src.at[:, span], dst.at[:, span], sem.at[1 + i * parts + k]))
    for c in copies:
        c.start()
    total = total_v[...]
    n_layer = ratio_v.shape[0]
    ratios = jnp.sqrt(total / (pltpu.roll(total, LANES - n_layer, 1) + 1.0))
    ratios = jnp.where(lax.broadcasted_iota(jnp.int32, ratios.shape, 1) < n_layer, ratios, 0.0)
    row_step = jnp.broadcast_to(jnp.sum(chosen_v[...] * ratios, axis=1, keepdims=True), chosen_v.shape)
    ratio_v[...] = ratios[0, :n_layer]
    copies.append(pltpu.make_async_copy(ratio_v, ratio_hbm, sem.at[0]))
    copies[-1].start()

    for k in range(parts):
        def step_piece(i, carry, k=k):
            outer = pl.ds(pl.multiple_of(k * width + i * LANES, LANES), LANES)
            stepped = p_v[:, outer].astype(jnp.float32) - row_step * upd[:, outer]
            newp_v[:, outer] = stepped.astype(jnp.bfloat16)
            return carry

        lax.fori_loop(0, width // LANES, step_piece, 0, unroll=4)
        span = pl.ds(k * width, width)
        c = pltpu.make_async_copy(newp_v.at[:, span], newp_hbm.at[:, span], sem.at[1 + 2 * parts + k])
        c.start()
        copies.append(c)
    for c in copies:
        c.wait()


def shards(grad_parts, params, moment_first, moment_second, block_layer, block_valid, decay):
    n_sec, n_shard = lax.axis_size("section"), lax.axis_size("shard")
    chips = n_shard // 2
    n_y = max(d for d in range(1, math.isqrt(chips) + 1) if chips % d == 0)
    n_x = chips // n_y
    rows, cols = params.shape[1:]
    n_layer = decay.shape[0]
    half = cols // 2
    cuts = tuple(half // LANES * c // CUTS[-1] * LANES for c in CUTS)
    bf16, f32 = jnp.bfloat16, jnp.float32
    dma = pltpu.SemaphoreType.DMA
    one_shot = ONE_SHOT and n_shard * n_sec <= 32
    n_lines = n_shard * n_sec if one_shot else n_shard
    grads = grad_parts.reshape(n_y, n_x, 2, rows, cols)
    any_spec = pl.BlockSpec(memory_space=pltpu.HBM)
    vmem = pl.BlockSpec(memory_space=pltpu.VMEM)
    held = pl.pallas_call(
        functools.partial(kernel, n_sec, n_y, n_x, cuts),
        out_shape=(
            pltpu.VMEM((rows, cols), bf16),
            pltpu.VMEM((rows, cols), f32),
            pltpu.VMEM((rows, cols), f32),
            pltpu.VMEM((rows, cols), f32),
            pltpu.VMEM((rows, LANES), f32),
            pltpu.VMEM((1, LANES), f32),
        ),
        in_specs=[any_spec] * 7,
        out_specs=(vmem,) * 6,
        scratch_shapes=[
            pltpu.VMEM((n_y, n_x, 2, rows, cols), bf16),
            pltpu.VMEM((n_y, n_x, rows, cols), bf16),
            pltpu.VMEM((rows, cols), f32),
            pltpu.VMEM((rows, cols), f32),
            pltpu.VMEM((n_x - 1, n_y, rows, half), bf16),
            pltpu.VMEM((n_y - 1, n_x, rows, half), bf16),
            pltpu.VMEM((n_y - 1, rows, half), bf16),
            pltpu.VMEM((n_x - 1, rows, half), bf16),
            pltpu.VMEM((n_y - 1, rows, half), bf16),
            pltpu.VMEM((n_x - 1, rows, half), bf16),
            pltpu.VMEM((n_x - 1, n_y, rows, cuts[0]), bf16),
            pltpu.VMEM((n_y - 1, n_x, rows, cuts[0]), bf16),
            pltpu.VMEM((n_x - 1, n_y, rows, cuts[SHIFT] - cuts[SHIFT - 1]), bf16),
            pltpu.VMEM((n_y - 1, n_x, rows, cuts[SHIFT] - cuts[SHIFT - 1]), bf16),
            pltpu.VMEM((n_lines, 1, LANES), f32),
            None if one_shot else pltpu.VMEM((n_sec, 1, LANES), f32),
            pltpu.SMEM(block_layer.shape, jnp.int32),
            pltpu.SMEM(block_valid.shape, jnp.int32),
            pltpu.SMEM(decay.shape, f32),
        ],
        compiler_params=pltpu.CompilerParams(
            collective_id=0, has_side_effects=True, vmem_limit_bytes=56 * 1024 * 1024
        ),
    )(grads, params[0], moment_first[0], moment_second[0], block_layer, block_valid, decay)
    out = pl.pallas_call(
        functools.partial(finish, PARTS),
        out_shape=(
            jax.ShapeDtypeStruct((rows, cols), bf16),
            jax.ShapeDtypeStruct((rows, cols), f32),
            jax.ShapeDtypeStruct((rows, cols), f32),
            jax.ShapeDtypeStruct((n_layer,), f32),
        ),
        in_specs=[vmem] * 6,
        out_specs=(any_spec,) * 4,
        scratch_shapes=[pltpu.VMEM((rows, cols), bf16), pltpu.VMEM((n_layer,), f32), dma((1 + 3 * PARTS,))],
        compiler_params=pltpu.CompilerParams(vmem_limit_bytes=8 * 1024 * 1024),
    )(*held)
    return (out[0][None], out[1][None], out[2][None], out[3])


def solution(mesh):
    placed = (
        P("section", "shard", None, None),
        P("section", "shard", None),
        P("section", "shard", None),
        P("section", "shard", None),
        P("section", "shard"),
        P("section", "shard"),
        P(),
    )
    return jax.shard_map(
        shards,
        mesh=mesh,
        in_specs=placed,
        out_specs=(
            P("section", "shard", None),
            P("section", "shard", None),
            P("section", "shard", None),
            P(),
        ),
        check_vma=False,
    )
```
